32 devices in a mesh: seq: 16 (over z, y, core), batch: 2 (over x).
Axes of the slice: x: 2, y: 2, z: 4, core: 2. Of those that a mesh axis runs over, the one named last changes fastest.
Arguments:
- hidden_in: bfloat16 [2, 4096, 2304], P('batch', 'seq'), may hold values from -6 to 6
- segment_ids: int32 [2, 4096], P('batch', 'seq'), may hold values from 0 to 15, never falling along the last dimension, each value on 1 to 512 neighbouring positions
- pre_gain: float32 [2304], replicated, may hold values from 0.25 to 1.75
- w_qkv: bfloat16 [2304, 2048], P('seq'), may hold values from -0.27083333 to 0.27083333
- w_out: bfloat16 [1024, 2304], P('seq'), may hold values from -0.1875 to 0.1875
- post_gain: float32 [2304], replicated, may hold values from 0.25 to 1.75
Outputs:
- layer_out: bfloat16 [2, 4096, 2304], P('batch', 'seq')
The draws below stay inside these ranges and needn't reach their ends.
Inputs may be any that keep to these rules, and one draw needn't show every extreme that they name: `segment_ids`: along each sequence the numbers never fall; a document is 1 to 512 positions long, and each sequence has one of exactly 512.
All inputs are finite; a program needn't handle non-finite values.
Results may differ from the reference program's by a relative error of at most 0.012.
The reference program's roundings to bfloat16 on the way (of `normed` and `attended`) count: a program that leaves them out, or rounds other values in their place, can miss the bound.
Values may be sent and summed in bfloat16 or wider, within the bound.
No kernel may reach another device: no remote copies, remote signals or barrier semaphores. Data moves between devices by JAX's collectives and lax.ppermute only.
A program may use at most 128 MiB of HBM per device.

```python
import math
import jax
import jax.numpy as jnp
import numpy as np
from jax import lax

D = 2304
Q_HEADS = 4
KV_HEADS = 2
HEAD = 256
WINDOW = 4096
DOCS = 16
TOK_DEV = 256
SEQ = 4096
BATCH = 2
QKV_W = 2048
ATT_W = 1024
DOC_MOST = 512


def draw_w_qkv(key, part):
    base_key = jax.random.fold_in(key, 11)
    pick_key = jax.random.fold_in(key, 12)
    base = jnp.clip(jax.random.normal(base_key, (D, QKV_W), jnp.float32), -3.0, 3.0)
    order = jax.random.permutation(pick_key, KV_HEADS)
    boosted = order < (KV_HEADS + 1) // 2
    columns = jnp.arange(QKV_W, dtype=jnp.int32)
    head_of = columns // HEAD
    group_of = jnp.where(head_of < Q_HEADS, head_of // (Q_HEADS // KV_HEADS), head_of - Q_HEADS)
    group_of = jnp.clip(group_of, 0, KV_HEADS - 1)
    is_value = head_of >= Q_HEADS + KV_HEADS
    factor = jnp.where(boosted[group_of] & jnp.logical_not(is_value), 4.0, 1.0).astype(jnp.float32)
    return (base * factor[None, :] * float(D) ** (-0.5)).astype(jnp.bfloat16)


def block_levels(stream_key, dims, cuts, least, high):
    def one(position, shards_of):
        steps = jax.random.uniform(jax.random.fold_in(jax.random.fold_in(stream_key, 6), position), (shards_of,), jnp.float32, least / len(cuts), high / len(cuts))
        return jnp.repeat(jnp.exp(steps), dims[position] // shards_of).reshape((-1,) + (1,) * (len(dims) - position - 1))

    factor_of = one(*cuts[0])
    for cut in cuts[1:]:
        factor_of = factor_of * one(*cut)
    return factor_of


def profile(count, total, limit, lean):
    weights = [(1 << 20) // math.isqrt(standing ** lean) + 1 for standing in range(2, count + 1)]
    rest, given = total - limit - (count - 1), [1] * (count - 1)
    while rest > 0:
        free = [i for i in range(count - 1) if given[i] < limit]
        whole, budget = sum([weights[i] for i in free]), rest
        for i in free:
            addition = min(limit - given[i], max(1, budget * weights[i] // whole), rest)
            given[i] = given[i] + addition
            rest = rest - addition
    return np.array([limit] + given)


def uneven(own_key, count, total, bound, skew):
    if count == 2:
        one = jax.random.randint(own_key, (), max(1, total - bound), min(bound, total - 1) + 1)
        return jnp.stack([one, total - one])
    sizes = jnp.asarray(profile(count, total, bound, skew), jnp.int32)
    pairs = (count - 1) // 2
    source_of, taker = sizes[1:1 + 2 * pairs:2], sizes[2:2 + 2 * pairs:2]
    margin = jnp.minimum(source_of - 1, bound - taker)
    passed = jax.random.randint(jax.random.fold_in(own_key, 1), (pairs,), 0, 1 << 20) % (margin + 1)
    sizes = sizes.at[1:1 + 2 * pairs:2].set(source_of - passed).at[2:2 + 2 * pairs:2].set(taker + passed)
    return sizes[jax.random.permutation(jax.random.fold_in(own_key, 2), count)]


def normal_values(own_key, dims, width, most, cuts=(), held_as=jnp.bfloat16):
    values = jax.random.normal(own_key, dims, jnp.float32) * width
    if len(cuts) > 0:
        values = block_levels(own_key, dims, cuts, -0.22, 0.18) * values
    return jnp.clip(values, min=-most, max=most).astype(held_as)


def setup_inputs(seed: int = 0) -> dict:
    arg_keys = jax.random.split(jax.random.key(seed), 7)
    hidden_in = normal_values(arg_keys[0], (BATCH, SEQ, D), 1.0, 6.0, ((0, 2), (1, 16)))
    segment_ids = jax.vmap(lambda own: jnp.searchsorted(jnp.cumsum(uneven(own, DOCS, SEQ, DOC_MOST, 2)), jnp.arange(SEQ), side="right"))(jax.random.split(arg_keys[1], BATCH)).reshape((BATCH, SEQ)).astype(jnp.int32)
    pre_gain = jnp.clip(1.0 + 0.15 * jax.random.normal(arg_keys[2], (D,), jnp.float32), 0.25, 1.75)
    w_qkv = draw_w_qkv(jax.random.fold_in(arg_keys[6], 71), 0)
    w_out = normal_values(arg_keys[4], (ATT_W, D), ATT_W ** -0.5, 0.1875, ((0, 16),))
    post_gain = jnp.clip(1.0 + 0.15 * jax.random.normal(arg_keys[5], (D,), jnp.float32), 0.25, 1.75)
    return dict(hidden_in=hidden_in, segment_ids=segment_ids, pre_gain=pre_gain, w_qkv=w_qkv, w_out=w_out, post_gain=post_gain)


EPS = 1e-06
CAP = 50.0

def rms_scale(values, gain):
    return values * lax.rsqrt(lax.optimization_barrier(jnp.mean(values * values, axis=-1, keepdims=True)) + EPS) * gain

def barrier_round(values):
    return lax.optimization_barrier(values.astype(jnp.bfloat16)).astype(jnp.float32)

def rotary(values, positions):
    head_size = values.shape[-1]
    half_dim = head_size // 2
    inverse = 1.0 / 10000.0 ** (jnp.arange(half_dim, dtype=jnp.float32) * 2.0 / head_size)
    angles = positions.astype(jnp.float32)[:, None] * inverse[None, :]
    shape = (values.shape[0],) + (1,) * (values.ndim - 2) + (half_dim,)
    cosine = jnp.cos(angles).reshape(shape)
    sine = jnp.sin(angles).reshape(shape)
    first_half = values[..., :half_dim]
    second_half = values[..., half_dim:]
    return jnp.concatenate([first_half * cosine - second_half * sine, second_half * cosine + first_half * sine], axis=-1)

def one_sequence(inputs, segment_row, pre_gain, w_qkv, w_out, post_gain):
    seq_len = inputs.shape[0]
    groups = Q_HEADS // KV_HEADS
    widened = inputs.astype(jnp.float32)
    normed = rms_scale(widened, pre_gain).astype(jnp.bfloat16)
    projected = jnp.dot(normed, w_qkv, preferred_element_type=jnp.float32)
    positions = jnp.arange(seq_len, dtype=jnp.int32)
    queries = rotary(projected[:, :Q_HEADS * HEAD].reshape(seq_len, KV_HEADS, groups, HEAD), positions)
    key_rows = rotary(projected[:, Q_HEADS * HEAD:(Q_HEADS + KV_HEADS) * HEAD].reshape(seq_len, KV_HEADS, HEAD), positions)
    value_rows = projected[:, (Q_HEADS + KV_HEADS) * HEAD:].reshape(seq_len, KV_HEADS, HEAD)
    query_full = barrier_round(queries)
    key_full = barrier_round(key_rows)
    value_full = barrier_round(value_rows)
    doc_numbers = jnp.arange(DOCS, dtype=jnp.int32)
    matches = segment_row[:, None] == doc_numbers[None, :]
    first_pos = lax.optimization_barrier(jnp.min(jnp.where(matches, positions[:, None], seq_len), axis=0)).astype(jnp.int32)
    starts = lax.optimization_barrier(jnp.sum(jnp.where(matches, first_pos[None, :], 0), axis=1)).astype(jnp.int32)
    key_pad = jnp.concatenate([jnp.zeros((WINDOW, KV_HEADS, HEAD), jnp.float32), key_full], axis=0)
    value_pad = jnp.concatenate([jnp.zeros((WINDOW, KV_HEADS, HEAD), jnp.float32), value_full], axis=0)
    scale = 1.0 / math.sqrt(HEAD)

    def block(index):
        qstart = (index * TOK_DEV).astype(jnp.int32)
        query_block = lax.dynamic_slice_in_dim(query_full, qstart, TOK_DEV, 0)
        key_block = lax.dynamic_slice_in_dim(key_pad, qstart, WINDOW + TOK_DEV, 0)
        value_block = lax.dynamic_slice_in_dim(value_pad, qstart, WINDOW + TOK_DEV, 0)
        start_block = lax.dynamic_slice_in_dim(starts, qstart, TOK_DEV, 0)
        query_pos = qstart + jnp.arange(TOK_DEV, dtype=jnp.int32)
        key_pos = qstart - WINDOW + jnp.arange(WINDOW + TOK_DEV, dtype=jnp.int32)
        scores = jnp.einsum('qhgd,khd->qhgk', query_block, key_block) * scale
        capped = CAP * jnp.tanh(scores / CAP)
        allowed = (key_pos[None, :] <= query_pos[:, None]) & (query_pos[:, None] - key_pos[None, :] < WINDOW) & (key_pos[None, :] >= start_block[:, None])
        weights = jnp.where(allowed[:, None, None, :], jnp.exp(capped), 0.0)
        totals = lax.optimization_barrier(jnp.sum(weights, axis=-1))
        mixed = jnp.einsum('qhgk,khd->qhgd', barrier_round(weights), value_block)
        return (mixed / totals[..., None]).astype(jnp.bfloat16).reshape(TOK_DEV, Q_HEADS * HEAD)
    attended = lax.map(block, jnp.arange(seq_len // TOK_DEV, dtype=jnp.int32)).reshape(seq_len, Q_HEADS * HEAD)
    branch = jnp.dot(attended, w_out, preferred_element_type=jnp.float32)
    return (widened + rms_scale(branch, post_gain)).astype(jnp.bfloat16)

def reference(hidden_in, segment_ids, pre_gain, w_qkv, w_out, post_gain):
    results = []
    for row in range(BATCH):
        results.append(one_sequence(hidden_in[row], segment_ids[row], pre_gain, w_qkv, w_out, post_gain))
    return jnp.stack(results, axis=0)
```

```python
import math

import jax
import jax.numpy as jnp
from jax import lax
from jax.sharding import PartitionSpec as P

Q_HEADS = 4
KV_HEADS = 2
HEAD = 256
WINDOW = 4096
DOCS = 16


EPS = 1e-06
CAP = 50.0


def from_behind(block, axis, distance):
    devices = range(lax.axis_size(axis))
    route = [(i - distance, i) for i in devices if i - distance in devices]
    return lax.ppermute(block, axis, route)


def rms_scale(values, gain):
    return values * lax.rsqrt(jnp.mean(values * values, axis=-1, keepdims=True) + EPS) * gain


def rotary(values, positions, leading):
    head_size = values.shape[-1]
    half_dim = head_size // 2
    inverse = 1.0 / 10000.0 ** (jnp.arange(half_dim, dtype=jnp.float32) * 2.0 / head_size)
    angles = positions.astype(jnp.float32)[:, None] * inverse[None, :]
    shape = (
        (1,) * leading + (positions.shape[0],) + (1,) * (values.ndim - 2 - leading) + (half_dim,)
    )
    cosine = jnp.cos(angles).reshape(shape)
    sine = jnp.sin(angles).reshape(shape)
    first_half = values[..., :half_dim]
    second_half = values[..., half_dim:]
    return jnp.concatenate(
        [first_half * cosine - second_half * sine, second_half * cosine + first_half * sine],
        axis=-1,
    )


def attend(states, queries, key_block, value_block, query_pos, key_pos, starts):
    running, totals = states
    scores = jnp.einsum(
        "qhgd,khd->qhgk", queries, key_block, preferred_element_type=jnp.float32
    ) * (1.0 / math.sqrt(HEAD))
    capped = CAP * jnp.tanh(scores / CAP)
    allowed = (
        (key_pos[None, :] <= query_pos[:, None])
        & (query_pos[:, None] - key_pos[None, :] < WINDOW)
        & (key_pos[None, :] >= starts[:, None])
    )
    weights = jnp.where(allowed[:, None, None, :], jnp.exp(capped), 0.0)
    totals = totals + jnp.sum(weights, axis=-1)
    running = running + jnp.einsum(
        "qhgk,khd->qhgd",
        weights.astype(jnp.bfloat16),
        value_block,
        preferred_element_type=jnp.float32,
    )
    return (running, totals)


def per_device(hidden_in, segment_ids, pre_gain, w_qkv, w_out, post_gain):
    tok_rows = hidden_in.shape[1]
    seq_count = lax.axis_size("seq")
    seq_index = lax.axis_index("seq")
    groups = Q_HEADS // KV_HEADS
    positions = seq_index * tok_rows + jnp.arange(tok_rows, dtype=jnp.int32)
    widened = hidden_in[0].astype(jnp.float32)
    normed = rms_scale(widened, pre_gain).astype(jnp.bfloat16)
    columns = normed
    projected = jnp.dot(
        columns,
        lax.all_gather(w_qkv, "seq", axis=0, tiled=True),
        preferred_element_type=jnp.float32,
    )
    queries = rotary(
        projected[:, : Q_HEADS * HEAD].reshape(tok_rows, KV_HEADS, groups, HEAD), positions, 0
    ).astype(jnp.bfloat16)
    key_rows = rotary(
        projected[:, Q_HEADS * HEAD : (Q_HEADS + KV_HEADS) * HEAD].reshape(
            tok_rows, KV_HEADS, HEAD
        ),
        positions,
        0,
    ).astype(jnp.bfloat16)
    value_rows = (
        projected[:, (Q_HEADS + KV_HEADS) * HEAD :]
        .reshape(tok_rows, KV_HEADS, HEAD)
        .astype(jnp.bfloat16)
    )
    doc_numbers = jnp.arange(DOCS, dtype=jnp.int32)
    matches = segment_ids[0][:, None] == doc_numbers[None, :]
    local_first = jnp.min(jnp.where(matches, positions[:, None], seq_count * tok_rows), axis=0)
    first_pos = lax.pmin(local_first, "seq")
    starts = jnp.sum(jnp.where(matches, first_pos[None, :], 0), axis=1)
    states = (
        jnp.zeros((tok_rows, KV_HEADS, groups, HEAD), jnp.float32),
        jnp.zeros((tok_rows, KV_HEADS, groups), jnp.float32),
    )
    states = attend(states, queries, key_rows, value_rows, positions, positions, starts)
    longest = min(2 * seq_count * tok_rows // DOCS, WINDOW)
    hop_count = min(-(-(longest - 1) // tok_rows), seq_count - 1)

    def relay_step(hop_index, carried):
        moving_keys, moving_values, running, totals = carried
        moving_keys, moving_values = from_behind((moving_keys, moving_values), "seq", 1)
        running, totals = attend(
            (running, totals),
            queries,
            moving_keys,
            moving_values,
            positions,
            positions - hop_index * tok_rows,
            starts,
        )
        return (moving_keys, moving_values, running, totals)

    carried = lax.fori_loop(
        1, hop_count + 1, relay_step, (key_rows, value_rows, states[0], states[1])
    )
    states = (carried[2], carried[3])
    running, totals = states
    attended = (running / totals[..., None]).astype(jnp.bfloat16).reshape(tok_rows, Q_HEADS * HEAD)
    columns = attended
    branch = jnp.dot(
        columns,
        lax.all_gather(w_out, "seq", axis=0, tiled=True),
        preferred_element_type=jnp.float32,
    )
    return (widened + rms_scale(branch, post_gain)).astype(jnp.bfloat16)[None]


def solution(mesh):
    placed = (P("batch", "seq", None), P("batch", "seq"), P(), P("seq", None), P("seq", None), P())
    return jax.shard_map(
        per_device, mesh=mesh, in_specs=placed, out_specs=P("batch", "seq", None), check_vma=False
    )
```

```python
import functools
import math

import jax
import jax.numpy as jnp
from jax import lax
from jax.experimental import pallas as pl
from jax.experimental.pallas import tpu as pltpu
from jax.sharding import PartitionSpec as P

Q_HEADS = 4
KV_HEADS = 2
HEAD = 256
WINDOW = 4096
DOCS = 16
EPS = 1e-06
CAP = 50.0
GROUPS = Q_HEADS // KV_HEADS


def rms_scale(values, gain):
    return values * lax.rsqrt(jnp.mean(values * values, axis=-1, keepdims=True) + EPS) * gain


def rotary_tables(positions):
    half_dim = HEAD // 2
    inverse = 1.0 / 10000.0 ** (jnp.arange(half_dim, dtype=jnp.float32) * 2.0 / HEAD)
    angles = positions.astype(jnp.float32)[:, None] * inverse[None, :]
    return jnp.cos(angles), jnp.sin(angles)


def swap_core(block):
    return lax.ppermute(block, "seq", [(i, i ^ 1) for i in range(lax.axis_size("seq"))])


def swap_pair(block):
    return lax.ppermute(block, "seq", [(i, i ^ 2) for i in range(lax.axis_size("seq"))])


def swap_batch(block):
    return lax.ppermute(block, "batch", [(0, 1), (1, 0)])


def along_line(block):
    count = lax.axis_size("seq")
    return lax.ppermute(block, "seq", [(i, (i + 4) % count) for i in range(count)])


def from_chip_behind(block, distance):
    count = lax.axis_size("seq")
    return lax.ppermute(
        block, "seq", [(i, i + 2 * distance) for i in range(count - 2 * distance)]
    )


def gather_wide(mine, rest, line_count):
    own = jnp.stack([mine, rest])
    pair_own = swap_pair(own)
    pieces = [
        (own, 0, (False, True), (False, False)),
        (pair_own, 0, (False, True), (True, True)),
    ]
    unit = jnp.stack([mine, pair_own[0]])
    for back in range(1, line_count):
        unit = along_line(unit)
        pieces.append((unit, back, (False, False), (False, True)))
        pieces.append((swap_batch(unit), back, (True, True), (False, True)))
    return pieces


def gather_narrow(mine, rest, line_count):
    own = jnp.stack([mine, rest])
    pair_own = swap_pair(own)
    pieces = [
        (own, 0, (False, True), (False, False)),
        (pair_own, 0, (False, True), (True, True)),
    ]
    unit = mine
    for back in range(1, line_count):
        unit = along_line(unit)
        other = swap_batch(unit)
        both = jnp.stack([unit, other])
        pieces.append((both, back, (False, True), (False, False)))
        pieces.append((swap_pair(both), back, (False, True), (True, True)))
    return pieces


def project_kernel(where, turned, spots, x_ref, cos_ref, sin_ref, *refs):
    count = len(where)
    pieces, out_ref, held, sems = refs[:count], refs[count], refs[count + 1], refs[count + 2]
    rows = pieces[0].shape[1]
    copies = []
    for piece, blocks in zip(pieces, where):
        for i in range(len(blocks)):
            at = pl.multiple_of(spots[len(copies)] * rows, rows)
            copies.append(
                pltpu.make_async_copy(
                    piece.at[i], held.at[pl.ds(at, rows), :], sems.at[len(copies)]
                )
            )
            copies[-1].start()
    for copy in copies:
        copy.wait()
    half = HEAD // 2
    step = 256

    def body(m, carry):
        tokens = pl.ds(pl.multiple_of(m * step, step), step)
        full = jnp.dot(x_ref[tokens, :], held[...], preferred_element_type=jnp.float32)
        cosine, sine = cos_ref[tokens, :], sin_ref[tokens, :]
        for h, turn in enumerate(turned):
            a = full[:, h * HEAD : h * HEAD + half]
            b = full[:, h * HEAD + half : (h + 1) * HEAD]
            if turn:
                a, b = a * cosine - b * sine, b * cosine + a * sine
            out_ref[tokens, h * HEAD : h * HEAD + half] = a.astype(jnp.bfloat16)
            out_ref[tokens, h * HEAD + half : (h + 1) * HEAD] = b.astype(jnp.bfloat16)
        return carry

    lax.fori_loop(0, x_ref.shape[0] // step, body, 0)


def project(x, cosine, sine, arrays, where, spots, turned):
    tokens, depth = x.shape
    width = arrays[0].shape[2]
    total = sum(len(blocks) for blocks in where)
    vmem = pl.BlockSpec(memory_space=pltpu.VMEM)
    return pl.pallas_call(
        functools.partial(project_kernel, where, turned),
        out_shape=jax.ShapeDtypeStruct((tokens, width), jnp.bfloat16),
        in_specs=[pl.BlockSpec(memory_space=pltpu.SMEM), vmem, vmem, vmem]
        + [pl.BlockSpec(memory_space=pl.ANY)] * len(arrays),
        out_specs=vmem,
        scratch_shapes=[
            pltpu.VMEM((depth, width), jnp.bfloat16),
            pltpu.SemaphoreType.DMA((total,)),
        ],
        compiler_params=pltpu.CompilerParams(vmem_limit_bytes=24 * 1024 * 1024),
        cost_estimate=pl.CostEstimate(
            flops=2 * tokens * depth * width, bytes_accessed=2 * depth * width, transcendentals=0
        ),
        name="project",
    )(spots, x, cosine, sine, *arrays)


def attend_kernel(behind, q_ref, kv_ref, old_ref, qseg_ref, kseg_ref, out_ref):
    tokens = q_ref.shape[0]
    step = out_ref.shape[2]
    for m in range(tokens // step):
        low = m * step
        top = behind + (m + 1) * step
        span = top - low
        qpos = behind + m * step + lax.broadcasted_iota(jnp.int32, (step, span), 0)
        kpos = low + lax.broadcasted_iota(jnp.int32, (step, span), 1)
        same = qseg_ref[m * step : (m + 1) * step, :] == kseg_ref[:, low:top]
        allowed = same & (kpos <= qpos) & (qpos - kpos < WINDOW)
        keys = jnp.concatenate([old_ref[low:, :HEAD], kv_ref[: (m + 1) * step, :HEAD]], axis=0)
        values = jnp.concatenate([old_ref[low:, HEAD:], kv_ref[: (m + 1) * step, HEAD:]], axis=0)
        for h in range(GROUPS):
            q = q_ref[m * step : (m + 1) * step, h * HEAD : (h + 1) * HEAD]
            scores = lax.dot_general(
                q, keys, (((1,), (1,)), ((), ())), preferred_element_type=jnp.float32
            ) * (1.0 / math.sqrt(HEAD))
            capped = CAP * jnp.tanh(scores / CAP)
            weights = jnp.where(allowed, jnp.exp(capped), 0.0)
            totals = jnp.sum(weights, axis=1, keepdims=True)
            mixed = jnp.dot(
                weights.astype(jnp.bfloat16), values, preferred_element_type=jnp.float32
            )
            out_ref[m, h] = (mixed / totals).astype(jnp.bfloat16)


def attend(q, kv, old, qseg, kseg, blocks):
    tokens = q.shape[0]
    behind = old.shape[0]
    work = GROUPS * tokens * (behind + tokens) * HEAD
    return pl.pallas_call(
        functools.partial(attend_kernel, behind),
        out_shape=jax.ShapeDtypeStruct((blocks, GROUPS, tokens // blocks, HEAD), jnp.bfloat16),
        in_specs=[pl.BlockSpec(memory_space=pltpu.VMEM)] * 5,
        out_specs=pl.BlockSpec(memory_space=pltpu.VMEM),
        compiler_params=pltpu.CompilerParams(vmem_limit_bytes=24 * 1024 * 1024),
        cost_estimate=pl.CostEstimate(flops=4 * work, bytes_accessed=work // 256, transcendentals=0),
        name="attend",
    )(q, kv, old, qseg, kseg)


def out_kernel(where, heads, last, marks, *refs):
    refs = list(refs)
    att_ref = refs.pop(0)
    if last:
        early_ref, hid_ref, gain_ref = refs.pop(0), refs.pop(0), refs.pop(0)
    count = len(where)
    pieces = refs[:count]
    out_ref, held, sum_ref, sems = refs[count:]
    rows = pieces[0].shape[1]
    copies = []
    for piece, blocks in zip(pieces, where):
        for i, slot in enumerate(blocks):
            at = pl.multiple_of(marks[heads + len(copies)], rows)
            copies.append(
                pltpu.make_async_copy(
                    piece.at[i], held.at[slot, pl.ds(at, rows), :], sems.at[len(copies)]
                )
            )
            copies[-1].start()
    for copy in copies:
        copy.wait()
    width = out_ref.shape[1]
    tile = next(t for t in (768, 512, 256, 128, width) if width % t == 0)
    if not last:
        for n in range(width // tile):
            part = slice(n * tile, (n + 1) * tile)
            total = jnp.zeros((out_ref.shape[0], tile), jnp.float32)
            for s in range(heads):
                total = total + jnp.dot(
                    att_ref[marks[s]], held[s, :, part], preferred_element_type=jnp.float32
                )
            out_ref[:, part] = total
        return
    square = jnp.zeros((out_ref.shape[0], 1), jnp.float32)
    for n in range(width // tile):
        part = slice(n * tile, (n + 1) * tile)
        total = early_ref[:, part]
        for s in range(heads):
            total = total + jnp.dot(
                att_ref[marks[s]], held[s, :, part], preferred_element_type=jnp.float32
            )
        sum_ref[:, part] = total
        square = square + jnp.sum(total * total, axis=1, keepdims=True)
    scale = lax.rsqrt(square / width + EPS)
    for n in range(width // tile):
        part = slice(n * tile, (n + 1) * tile)
        branch = sum_ref[:, part] * scale * gain_ref[:, part]
        out_ref[:, part] = (hid_ref[:, part].astype(jnp.float32) + branch).astype(jnp.bfloat16)


def out_project(att, arrays, where, marks, heads, rows, finish=None):
    width = arrays[0].shape[2]
    tokens = att.shape[1]
    total = sum(len(blocks) for blocks in where)
    vmem = pl.BlockSpec(memory_space=pltpu.VMEM)
    extra = list(finish) if finish else []
    return pl.pallas_call(
        functools.partial(out_kernel, where, heads, bool(finish)),
        out_shape=jax.ShapeDtypeStruct((tokens, width), jnp.bfloat16 if finish else jnp.float32),
        in_specs=[pl.BlockSpec(memory_space=pltpu.SMEM)]
        + [vmem] * (1 + len(extra))
        + [pl.BlockSpec(memory_space=pl.ANY)] * len(arrays),
        out_specs=vmem,
        scratch_shapes=[
            pltpu.VMEM((heads, rows, width), jnp.bfloat16),
            pltpu.VMEM((tokens, width) if finish else (8, 128), jnp.float32),
            pltpu.SemaphoreType.DMA((total,)),
        ],
        compiler_params=pltpu.CompilerParams(vmem_limit_bytes=24 * 1024 * 1024),
        cost_estimate=pl.CostEstimate(
            flops=2 * tokens * rows * heads * width, bytes_accessed=2 * rows * heads * width,
            transcendentals=0,
        ),
        name="finish" if finish else "early",
    )(marks, att, *extra, *arrays)


def per_device(hidden_in, segment_ids, pre_gain, w_qkv, w_out, post_gain):
    tok_rows, model = hidden_in.shape[1:]
    seq_count = lax.axis_size("seq")
    line_count = seq_count // 4
    seq_index = lax.axis_index("seq")
    plane = lax.axis_index("batch")
    core, pair, line = seq_index % 2, (seq_index // 2) % 2, seq_index // 4
    chip = seq_index // 2
    chip_rows = 2 * tok_rows
    on_plane = plane == core

    att_w = Q_HEADS * HEAD
    group_w = GROUPS * HEAD

    def columns_of(c):
        return jnp.concatenate(
            [
                lax.dynamic_slice_in_dim(w_qkv, att_w + c * HEAD, HEAD, 1),
                lax.dynamic_slice_in_dim(w_qkv, att_w + (KV_HEADS + c) * HEAD, HEAD, 1),
                lax.dynamic_slice_in_dim(w_qkv, c * group_w, group_w, 1),
            ],
            axis=1,
        )

    kept = columns_of(core)
    came = swap_core(columns_of(1 - core))
    mine = jnp.where(on_plane, kept, came)
    rest = jnp.where(on_plane, came, kept)
    kv_pieces = gather_narrow(mine[:, : 2 * HEAD], rest[:, : 2 * HEAD], line_count)

    def by_core(own, other):
        return jnp.where(
            core == 0, jnp.concatenate([own, other]), jnp.concatenate([other, own])
        )

    hidden_chip = by_core(hidden_in[0], swap_core(hidden_in[0]))
    normed = rms_scale(hidden_chip.astype(jnp.float32), pre_gain).astype(jnp.bfloat16)
    ids = by_core(segment_ids[0], swap_core(segment_ids[0]))
    longest = min(2 * seq_count * tok_rows // DOCS, WINDOW)
    hops = min(-(-(longest - 1) // chip_rows), seq_count // 2 - 1)
    key_ids = [
        jnp.where(chip >= d, from_chip_behind(ids, d), -1) for d in range(hops, 0, -1)
    ] + [ids]
    cosine, sine = rotary_tables(chip * chip_rows + jnp.arange(chip_rows, dtype=jnp.int32))

    def spot(back, other_half, other_pair):
        layer = (line - back + line_count) % line_count
        y = 1 - pair if other_pair else pair
        h = 1 - plane if other_half else plane
        return layer, y, h

    def projected(pieces, turned):
        spots, arrays, where = [], [], []
        for block, back, halves, pairs in pieces:
            arrays.append(block)
            where.append(tuple(range(len(halves))))
            for half, other in zip(halves, pairs):
                layer, y, h = spot(back, half, other)
                spots.append((layer * 2 + y) * 2 + h)
        spots = jnp.stack(spots).astype(jnp.int32)
        return project(normed, cosine, sine, arrays, tuple(where), spots, turned)

    q_pieces = gather_wide(mine[:, 2 * HEAD :], rest[:, 2 * HEAD :], line_count)
    kv = projected(kv_pieces, (True, False))
    old = jnp.concatenate([from_chip_behind(kv, d) for d in range(hops, 0, -1)])

    half_rows = w_out.shape[0] // 2
    out_mine = lax.dynamic_slice_in_dim(w_out, plane * half_rows, half_rows, 0)
    out_rest = lax.dynamic_slice_in_dim(w_out, (1 - plane) * half_rows, half_rows, 0)
    out_pieces = gather_wide(out_mine, out_rest, line_count)

    q = projected(q_pieces, (True, True))
    att = attend(q, kv, old, ids[:, None], jnp.concatenate(key_ids)[None, :], 2)
    att_own = lax.dynamic_index_in_dim(att, core, 0, keepdims=False)
    att_other = swap_core(lax.dynamic_index_in_dim(att, 1 - core, 0, keepdims=False))
    att = by_core(att_own, att_other)

    def out_part(backs, finish=None):
        heads = [(line - back + line_count) % line_count for back in backs]
        offsets, arrays, where = [], [], []
        for block, back, halves, pairs in out_pieces:
            if back not in backs:
                continue
            for array, c in ((block, core), (swap_core(block), 1 - core)):
                arrays.append(array)
                where.append((backs.index(back),) * len(halves))
                for half, other in zip(halves, pairs):
                    _, y, h = spot(back, half, other)
                    offsets.append(((y * 2 + c) * 2 + h) * half_rows)
        marks = jnp.stack(heads + offsets).astype(jnp.int32)
        return out_project(
            att, arrays, tuple(where), marks, len(backs), 8 * half_rows, finish
        )

    early = out_part(list(range(line_count - 1)))
    done = out_part([line_count - 1], (early, hidden_in[0], post_gain[None, :]))
    return done[None]


def from_behind(block, axis, distance):
    devices = range(lax.axis_size(axis))
    route = [(i - distance, i) for i in devices if i - distance in devices]
    return lax.ppermute(block, axis, route)


def rotary(values, positions, leading):
    head_size = values.shape[-1]
    half_dim = head_size // 2
    inverse = 1.0 / 10000.0 ** (jnp.arange(half_dim, dtype=jnp.float32) * 2.0 / head_size)
    angles = positions.astype(jnp.float32)[:, None] * inverse[None, :]
    shape = (
        (1,) * leading + (positions.shape[0],) + (1,) * (values.ndim - 2 - leading) + (half_dim,)
    )
    cosine = jnp.cos(angles).reshape(shape)
    sine = jnp.sin(angles).reshape(shape)
    first_half = values[..., :half_dim]
    second_half = values[..., half_dim:]
    return jnp.concatenate(
        [first_half * cosine - second_half * sine, second_half * cosine + first_half * sine],
        axis=-1,
    )


def attend_block(states, queries, key_block, value_block, query_pos, key_pos, starts):
    running, totals = states
    scores = jnp.einsum(
        "qhgd,khd->qhgk", queries, key_block, preferred_element_type=jnp.float32
    ) * (1.0 / math.sqrt(HEAD))
    capped = CAP * jnp.tanh(scores / CAP)
    allowed = (
        (key_pos[None, :] <= query_pos[:, None])
        & (query_pos[:, None] - key_pos[None, :] < WINDOW)
        & (key_pos[None, :] >= starts[:, None])
    )
    weights = jnp.where(allowed[:, None, None, :], jnp.exp(capped), 0.0)
    totals = totals + jnp.sum(weights, axis=-1)
    running = running + jnp.einsum(
        "qhgk,khd->qhgd",
        weights.astype(jnp.bfloat16),
        value_block,
        preferred_element_type=jnp.float32,
    )
    return (running, totals)


def per_device_general(hidden_in, segment_ids, pre_gain, w_qkv, w_out, post_gain):
    tok_rows = hidden_in.shape[1]
    seq_count = lax.axis_size("seq")
    seq_index = lax.axis_index("seq")
    groups = Q_HEADS // KV_HEADS
    positions = seq_index * tok_rows + jnp.arange(tok_rows, dtype=jnp.int32)
    widened = hidden_in[0].astype(jnp.float32)
    normed = rms_scale(widened, pre_gain).astype(jnp.bfloat16)
    columns = normed
    projected = jnp.dot(
        columns,
        lax.all_gather(w_qkv, "seq", axis=0, tiled=True),
        preferred_element_type=jnp.float32,
    )
    queries = rotary(
        projected[:, : Q_HEADS * HEAD].reshape(tok_rows, KV_HEADS, groups, HEAD), positions, 0
    ).astype(jnp.bfloat16)
    key_rows = rotary(
        projected[:, Q_HEADS * HEAD : (Q_HEADS + KV_HEADS) * HEAD].reshape(
            tok_rows, KV_HEADS, HEAD
        ),
        positions,
        0,
    ).astype(jnp.bfloat16)
    value_rows = (
        projected[:, (Q_HEADS + KV_HEADS) * HEAD :]
        .reshape(tok_rows, KV_HEADS, HEAD)
        .astype(jnp.bfloat16)
    )
    doc_numbers = jnp.arange(DOCS, dtype=jnp.int32)
    matches = segment_ids[0][:, None] == doc_numbers[None, :]
    local_first = jnp.min(jnp.where(matches, positions[:, None], seq_count * tok_rows), axis=0)
    first_pos = lax.pmin(local_first, "seq")
    starts = jnp.sum(jnp.where(matches, first_pos[None, :], 0), axis=1)
    states = (
        jnp.zeros((tok_rows, KV_HEADS, groups, HEAD), jnp.float32),
        jnp.zeros((tok_rows, KV_HEADS, groups), jnp.float32),
    )
    states = attend_block(states, queries, key_rows, value_rows, positions, positions, starts)
    longest = min(2 * seq_count * tok_rows // DOCS, WINDOW)
    hop_count = min(-(-(longest - 1) // tok_rows), seq_count - 1)

    def relay_step(hop_index, carried):
        moving_keys, moving_values, running, totals = carried
        moving_keys, moving_values = from_behind((moving_keys, moving_values), "seq", 1)
        running, totals = attend_block(
            (running, totals),
            queries,
            moving_keys,
            moving_values,
            positions,
            positions - hop_index * tok_rows,
            starts,
        )
        return (moving_keys, moving_values, running, totals)

    carried = lax.fori_loop(
        1, hop_count + 1, relay_step, (key_rows, value_rows, states[0], states[1])
    )
    states = (carried[2], carried[3])
    running, totals = states
    attended = (running / totals[..., None]).astype(jnp.bfloat16).reshape(tok_rows, Q_HEADS * HEAD)
    columns = attended
    branch = jnp.dot(
        columns,
        lax.all_gather(w_out, "seq", axis=0, tiled=True),
        preferred_element_type=jnp.float32,
    )
    return (widened + rms_scale(branch, post_gain)).astype(jnp.bfloat16)[None]


def solution(mesh):
    seq_count, planes = mesh.shape["seq"], mesh.shape["batch"]
    special = seq_count == 4 * Q_HEADS and planes == 2 and KV_HEADS == 2
    placed = (P("batch", "seq", None), P("batch", "seq"), P(), P("seq", None), P("seq", None), P())
    return jax.shard_map(
        per_device if special else per_device_general,
        mesh=mesh,
        in_specs=placed,
        out_specs=P("batch", "seq", None),
        check_vma=False,
    )
```

```python
import functools
import math

import jax
import jax.numpy as jnp
from jax import lax
from jax.experimental import pallas as pl
from jax.experimental.pallas import tpu as pltpu
from jax.sharding import PartitionSpec as P


Q_HEADS = 4
KV_HEADS = 2
HEAD = 256
WINDOW = 4096
DOCS = 16
EPS = 1e-06
CAP = 50.0
TAIL = 16
GROUPS = Q_HEADS // KV_HEADS


def rms_scale(values, gain):
    return values * lax.rsqrt(jnp.mean(values * values, axis=-1, keepdims=True) + EPS) * gain


def rotary_tables(positions):
    half_dim = HEAD // 2
    inverse = 1.0 / 10000.0 ** (jnp.arange(half_dim, dtype=jnp.float32) * 2.0 / HEAD)
    angles = positions.astype(jnp.float32)[:, None] * inverse[None, :]
    return jnp.cos(angles), jnp.sin(angles)


def swap_core(block):
    return lax.ppermute(block, "seq", [(i, i ^ 1) for i in range(lax.axis_size("seq"))])


def swap_pair(block):
    return lax.ppermute(block, "seq", [(i, i ^ 2) for i in range(lax.axis_size("seq"))])


def swap_batch(block):
    return lax.ppermute(block, "batch", [(0, 1), (1, 0)])


def along_line(block, steps):
    count = lax.axis_size("seq")
    return lax.ppermute(block, "seq", [(i, (i + 4 * steps) % count) for i in range(count)])


def from_chip_behind(block, distance):
    count = lax.axis_size("seq")
    return lax.ppermute(block, "seq", [(i, (i + 2 * distance) % count) for i in range(count)])


def line_gather(unit, line_count):
    units = []
    for _ in range(1, line_count):
        unit = along_line(unit, 1)
        units.append(unit)
    return units


def gather_near(own, unit, plane, pair, line_count, tag):
    pair_own = swap_pair(own)
    pieces = [(own, [(0, pair, 0), (0, pair, 1)]), (pair_own, [(0, 1 - pair, 0), (0, 1 - pair, 1)])]
    first, second, third = line_gather(unit, line_count)
    near = pack(first, second[None], 0)
    for name, block, backs in (("n", near, (1, 2)), ("f", third[None], (3,))):
        pieces.append((block, [(k, pair, plane) for k in backs]))
        beside = swap_batch(block)
        pieces.append((beside, [(k, pair, 1 - plane) for k in backs]))
        across = swap_pair(block)
        pieces.append((across, [(k, 1 - pair, plane) for k in backs]))
        if tag + name in BY_BATCH:
            corner = swap_batch(across)
        else:
            corner = swap_pair(beside)
        pieces.append((corner, [(k, 1 - pair, 1 - plane) for k in backs]))
    return pieces


def gather_wide(own, mine, plane, pair, line_count):
    pair_own = swap_pair(own)
    pieces = [(own, [(0, pair, 0), (0, pair, 1)]), (pair_own, [(0, 1 - pair, 0), (0, 1 - pair, 1)])]
    unit = pack(mine, pair_own, plane)
    for back, block in enumerate(line_gather(unit, line_count), 1):
        pieces.append((block, [(back, pair, plane), (back, 1 - pair, plane)]))
        other = swap_batch(block)
        pieces.append((other, [(back, pair, 1 - plane), (back, 1 - pair, 1 - plane)]))
    return pieces


def in_hbm(arrays):
    return [pltpu.with_memory_space_constraint(array, pltpu.HBM) for array in arrays]


def pack_kernel(place, first_ref, second_ref, out_ref):
    out_ref[0] = first_ref[...]
    out_ref[1] = second_ref[place[0]]


def pack(first, second, index):
    vmem = pl.BlockSpec(memory_space=pltpu.VMEM)
    return pl.pallas_call(
        pack_kernel,
        out_shape=jax.ShapeDtypeStruct((2,) + first.shape, first.dtype),
        in_specs=[pl.BlockSpec(memory_space=pltpu.SMEM)] + [vmem] * 2,
        out_specs=vmem,
        compiler_params=pltpu.CompilerParams(vmem_limit_bytes=4 * 1024 * 1024),
        cost_estimate=pl.CostEstimate(flops=1000000, bytes_accessed=6 * first.size, transcendentals=0),
        name="pack",
    )(jnp.asarray(index, jnp.int32)[None], first, second)


def prepare_kernel(place, w_ref, came_ref, out_ref, kv_ref, q_ref, kv_unit, q_unit, out_unit):
    core, plane = place[0], place[1]
    rows = out_ref.shape[0] // 2
    at_q = pl.multiple_of(core * GROUPS * HEAD, 128)
    at_k = pl.multiple_of((Q_HEADS + core) * HEAD, 128)
    at_v = pl.multiple_of((Q_HEADS + KV_HEADS + core) * HEAD, 128)
    out_unit[...] = out_ref[pl.ds(pl.multiple_of(plane * rows, rows), rows), :]
    for ref, half in ((w_ref, core), (came_ref, 1 - core)):
        for target, low, at, width in (
            (kv_ref, 0, at_k, HEAD),
            (kv_ref, HEAD, at_v, HEAD),
            (q_ref, 0, at_q, GROUPS * HEAD),
        ):
            block = ref[:, pl.ds(at, width)]
            target[half, :, low : low + width] = block
            unit = kv_unit if target is kv_ref else q_unit

            @pl.when(half == plane)
            def _():
                unit[:, low : low + width] = block


def prepare(w_qkv, came, w_out, core, plane):
    rows = w_qkv.shape[0]
    vmem = pl.BlockSpec(memory_space=pltpu.VMEM)
    kv, q = 2 * HEAD, GROUPS * HEAD
    return pl.pallas_call(
        prepare_kernel,
        out_shape=[
            jax.ShapeDtypeStruct(shape, jnp.bfloat16)
            for shape in (
                (2, rows, kv),
                (2, rows, q),
                (rows, kv),
                (rows, q),
                (w_out.shape[0] // 2, w_out.shape[1]),
            )
        ],
        in_specs=[pl.BlockSpec(memory_space=pltpu.SMEM)] + [vmem] * 3,
        out_specs=[vmem] * 5,
        compiler_params=pltpu.CompilerParams(vmem_limit_bytes=12 * 1024 * 1024),
        cost_estimate=pl.CostEstimate(flops=1000000, bytes_accessed=2 * w_qkv.size, transcendentals=0),
        name="prepare",
    )(jnp.stack([core, plane]).astype(jnp.int32), *in_hbm([w_qkv]), came, *in_hbm([w_out]))


def norm_kernel(in_ref, gain_ref, cos_ref, sin_ref, out_ref):
    step = 64

    def body(i, carry):
        at = pl.ds(pl.multiple_of(i * step, step), step)
        normed = rms_scale(in_ref[at, :].astype(jnp.float32), gain_ref[...]).astype(jnp.bfloat16)
        depth = normed.shape[1] // out_ref.shape[0]
        for part in range(out_ref.shape[0]):
            out_ref[part, at, :depth] = normed[:, part * depth : (part + 1) * depth]
        return carry

    lax.fori_loop(0, in_ref.shape[0] // step, body, 0)


def norm(rows, gain, tables, parts):
    count, width = rows.shape
    vmem = pl.BlockSpec(memory_space=pltpu.VMEM)
    return pl.pallas_call(
        norm_kernel,
        out_shape=jax.ShapeDtypeStruct((parts, count, -(-width // parts // 128) * 128), jnp.bfloat16),
        in_specs=[vmem] * 2 + [pl.BlockSpec(memory_space=pl.ANY)] * 2,
        out_specs=vmem,
        compiler_params=pltpu.CompilerParams(vmem_limit_bytes=8 * 1024 * 1024),
        cost_estimate=pl.CostEstimate(flops=1000000, bytes_accessed=4 * rows.size, transcendentals=0),
        name="norm",
    )(*in_hbm([rows]), gain[None, :], *in_hbm(tables))


def project_kernel(slots, turned, joined, early, spots, x_ref, other_ref, *refs):
    refs = list(refs)
    if joined:
        sum_ref = refs.pop(0)
    if not early:
        cos_ref, sin_ref = refs.pop(0), refs.pop(0)
    tailed = turned is not None and not all(turned)
    if tailed:
        ids_ref, other_ids_ref = refs.pop(0), refs.pop(0)
    pieces = refs[: len(slots)]
    out_ref, held, total, sems = refs[len(slots) :]
    layers = held.shape[0]
    rows = pieces[0].shape[1]
    copies = []
    for piece, blocks in zip(pieces, slots):
        for i, slot in enumerate(blocks):
            at = pl.multiple_of(spots[layers + len(copies)] * rows, rows)
            copy = pltpu.make_async_copy(
                piece.at[i], held.at[slot, pl.ds(at, rows), :], sems.at[len(copies)]
            )
            copy.start()
            copies.append((slot, copy))
    core = spots[layers + len(copies)]
    tokens = x_ref.shape[1]
    mine = pl.ds(pl.multiple_of(core * tokens, tokens), tokens)
    theirs = pl.ds(pl.multiple_of((1 - core) * tokens, tokens), tokens)
    if tailed:
        for ref, at in ((ids_ref, mine), (other_ids_ref, theirs)):
            row = jnp.broadcast_to(ref[...].astype(jnp.float32), (TAIL, tokens))
            out_ref[2 * tokens :, at] = row.astype(jnp.bfloat16)
    half = HEAD // 2
    for layer in range(layers):
        for slot, copy in copies:
            if slot == layer:
                copy.wait()
        last = layer == layers - 1
        for ref, at in ((x_ref, mine), (other_ref, theirs)):
            part = jnp.dot(
                ref[spots[layer], :, : held.shape[1]], held[layer], preferred_element_type=jnp.float32
            )
            if layer > 0:
                part = part + total[at, :]
            elif joined:
                part = part + sum_ref[at, :]
            if not last:
                total[at, :] = part
            elif early:
                out_ref[at, :] = part
            else:
                cosine, sine = cos_ref[at, :], sin_ref[at, :]
                for h, turn in enumerate(turned):
                    a = part[:, h * HEAD : h * HEAD + half]
                    b = part[:, h * HEAD + half : (h + 1) * HEAD]
                    if turn:
                        a, b = a * cosine - b * sine, b * cosine + a * sine
                    out_ref[at, h * HEAD : h * HEAD + half] = a.astype(jnp.bfloat16)
                    out_ref[at, h * HEAD + half : (h + 1) * HEAD] = b.astype(jnp.bfloat16)


def project(x, other, arrays, slots, layers, spots, turned=None, tables=(), before=None, ids=()):
    tokens, depth = 2 * x.shape[1], 4 * arrays[0].shape[1]
    width = arrays[0].shape[2]
    early = turned is None
    extra = ([] if before is None else [before]) + in_hbm(tables) + list(ids)
    vmem = pl.BlockSpec(memory_space=pltpu.VMEM)
    return pl.pallas_call(
        functools.partial(project_kernel, slots, turned, before is not None, early),
        out_shape=jax.ShapeDtypeStruct(
            (tokens + (TAIL if ids else 0), width), jnp.float32 if early else jnp.bfloat16
        ),
        in_specs=[pl.BlockSpec(memory_space=pltpu.SMEM)]
        + [vmem] * (2 + len(extra))
        + [pl.BlockSpec(memory_space=pl.ANY)] * len(arrays),
        out_specs=vmem,
        scratch_shapes=[
            pltpu.VMEM((layers, depth, width), jnp.bfloat16),
            pltpu.VMEM((tokens, width), jnp.float32),
            pltpu.SemaphoreType.DMA((sum(len(blocks) for blocks in slots),)),
        ],
        compiler_params=pltpu.CompilerParams(vmem_limit_bytes=12 * 1024 * 1024),
        cost_estimate=pl.CostEstimate(
            flops=2 * tokens * depth * layers * width,
            bytes_accessed=2 * layers * depth * width,
            transcendentals=0,
        ),
        name="project",
    )(spots, x, other, *extra, *in_hbm(arrays))


def attend_kernel(slots, place, x_ref, other_ref, sum_ref, cos_ref, sin_ref, ids_ref, *refs):
    other_ids_ref, kv_hbm, old_hbm = refs[:3]
    pieces = refs[3 : 3 + len(slots)]
    own_ref, send_ref, held, q_ref, kv_ref, old_ref, sems, ends = refs[3 + len(slots) :]
    rows = pieces[0].shape[1]
    copies = []
    for piece, blocks in zip(pieces, slots):
        for i in range(blocks):
            at = pl.multiple_of(place[3 + len(copies)] * rows, rows)
            copies.append(
                pltpu.make_async_copy(piece.at[i], held.at[pl.ds(at, rows), :], sems.at[len(copies)])
            )
            copies[-1].start()
    fetch = (
        pltpu.make_async_copy(kv_hbm, kv_ref, ends.at[0]),
        pltpu.make_async_copy(old_hbm, old_ref, ends.at[1]),
    )
    for copy in fetch:
        copy.start()
    core, chip, layer = place[0], place[1], place[2]
    step = own_ref.shape[1]
    tokens = q_ref.shape[0]
    behind = tokens
    first = core == 0
    ids = jnp.concatenate(
        [
            jnp.where(first, ids_ref[...], other_ids_ref[...]),
            jnp.where(first, other_ids_ref[...], ids_ref[...]),
        ],
        axis=1,
    ).astype(jnp.float32)
    query_ids = jnp.broadcast_to(ids, (128, tokens)).T[:, :1]
    half = HEAD // 2
    for copy in copies:
        copy.wait()
    for ref, block in ((x_ref, core), (other_ref, 1 - core)):
        at = pl.ds(pl.multiple_of(block * step, step), step)
        part = sum_ref[at, :] + jnp.dot(
            ref[layer, :, : held.shape[0]], held[...], preferred_element_type=jnp.float32
        )
        cosine, sine = cos_ref[at, :], sin_ref[at, :]
        for h in range(GROUPS):
            a = part[:, h * HEAD : h * HEAD + half]
            b = part[:, h * HEAD + half : (h + 1) * HEAD]
            q_ref[at, h * HEAD : h * HEAD + half] = (a * cosine - b * sine).astype(jnp.bfloat16)
            q_ref[at, h * HEAD + half : (h + 1) * HEAD] = (b * cosine + a * sine).astype(
                jnp.bfloat16
            )
    for copy in fetch:
        copy.wait()
    old_ids = old_ref[behind : behind + TAIL, :].astype(jnp.float32)[:1]
    key_ids = jnp.concatenate([jnp.where(chip > 0, old_ids, -1.0), ids], axis=1)
    for m in range(tokens // step):
        low = m * step
        top = behind + (m + 1) * step
        span = top - low
        qpos = behind + m * step + lax.broadcasted_iota(jnp.int32, (step, span), 0)
        kpos = low + lax.broadcasted_iota(jnp.int32, (step, span), 1)
        same = query_ids[m * step : (m + 1) * step, :] == key_ids[:, low:top]
        allowed = same & (kpos <= qpos) & (qpos - kpos < WINDOW)
        keys = jnp.concatenate([old_ref[low:behind, :HEAD], kv_ref[: (m + 1) * step, :HEAD]], axis=0)
        values = jnp.concatenate(
            [old_ref[low:behind, HEAD:], kv_ref[: (m + 1) * step, HEAD:]], axis=0
        )
        for h in range(GROUPS):
            q = q_ref[m * step : (m + 1) * step, h * HEAD : (h + 1) * HEAD]
            scores = lax.dot_general(
                q, keys, (((1,), (1,)), ((), ())), preferred_element_type=jnp.float32
            )
            capped = CAP * jnp.tanh(scores * (1.0 / (CAP * math.sqrt(HEAD))))
            weights = jnp.where(allowed, jnp.exp(capped), 0.0)
            totals = jnp.sum(weights, axis=1, keepdims=True)
            mixed = jnp.dot(
                weights.astype(jnp.bfloat16), values, preferred_element_type=jnp.float32
            )
            result = (mixed / totals).astype(jnp.bfloat16)

            @pl.when(core == m)
            def _():
                own_ref[h] = result

            @pl.when(core != m)
            def _():
                send_ref[h] = result


def attend(x, other, arrays, slots, place, before, tables, kv, old, ids):
    tokens, width = before.shape
    depth = 4 * arrays[0].shape[1]
    work = GROUPS * tokens * 2 * tokens * HEAD
    vmem, left = pl.BlockSpec(memory_space=pltpu.VMEM), pl.BlockSpec(memory_space=pl.ANY)
    return pl.pallas_call(
        functools.partial(attend_kernel, slots),
        out_shape=[jax.ShapeDtypeStruct((GROUPS, tokens // 2, HEAD), jnp.bfloat16)] * 2,
        in_specs=[pl.BlockSpec(memory_space=pltpu.SMEM)] + [vmem] * 7 + [left] * (2 + len(arrays)),
        out_specs=[vmem] * 2,
        scratch_shapes=[
            pltpu.VMEM((depth, width), jnp.bfloat16),
            pltpu.VMEM((tokens, width), jnp.bfloat16),
            pltpu.VMEM(kv.shape, jnp.bfloat16),
            pltpu.VMEM(old.shape, jnp.bfloat16),
            pltpu.SemaphoreType.DMA((sum(slots),)),
            pltpu.SemaphoreType.DMA((2,)),
        ],
        compiler_params=pltpu.CompilerParams(vmem_limit_bytes=16 * 1024 * 1024),
        cost_estimate=pl.CostEstimate(
            flops=4 * work, bytes_accessed=work // 256, transcendentals=0
        ),
        name="attend",
    )(place, x, other, before, *in_hbm(tables), *ids, *in_hbm([kv, old]), *in_hbm(arrays))


def fetch_layers(slots, first, marks, pieces, held, sems):
    rows = pieces[0].shape[1]
    copies = []
    for piece, blocks in zip(pieces, slots):
        for i, slot in enumerate(blocks):
            at = pl.multiple_of(marks[first + len(copies)], rows)
            copy = pltpu.make_async_copy(
                piece.at[i], held.at[slot, pl.ds(at, rows), :], sems.at[len(copies)]
            )
            copy.start()
            copies.append((slot, copy))
    return copies


def fetch_heads(own_hbm, other_hbm, own_ref, other_ref, ends):
    copies = (
        pltpu.make_async_copy(own_hbm, own_ref, ends.at[0]),
        pltpu.make_async_copy(other_hbm, other_ref, ends.at[1]),
    )
    for copy in copies:
        copy.start()
    return copies


def head_of(own_ref, other_ref, core, head):
    return jnp.where(head // GROUPS == core, own_ref[head % GROUPS], other_ref[head % GROUPS])


def early_kernel(slots, heads, marks, own_hbm, other_hbm, *refs):
    pieces = refs[: len(slots)]
    out_ref, held, own_ref, other_ref, sems, ends = refs[len(slots) :]
    fetch = fetch_heads(own_hbm, other_hbm, own_ref, other_ref, ends)
    copies = fetch_layers(slots, heads + 1, marks, pieces, held, sems)
    for copy in fetch:
        copy.wait()
    width = out_ref.shape[1]
    tile = next(t for t in (768, 512, 256, 128, width) if width % t == 0)
    for s in range(heads):
        for slot, copy in copies:
            if slot == s:
                copy.wait()
        att = head_of(own_ref, other_ref, marks[heads], marks[s])
        for n in range(width // tile):
            part = slice(n * tile, (n + 1) * tile)
            product = jnp.dot(att, held[s, :, part], preferred_element_type=jnp.float32)
            out_ref[:, part] = product if s == 0 else out_ref[:, part] + product


def finish_kernel(slots, marks, own_hbm, other_hbm, early_ref, gain_ref, hid_hbm, *refs):
    pieces = refs[: len(slots)]
    out_hbm, held, own_ref, other_ref, hid_ref, sum_ref, out_ref, sems, ends = refs[len(slots) :]
    heads = fetch_heads(own_hbm, other_hbm, own_ref, other_ref, ends)
    fetch = pltpu.make_async_copy(hid_hbm, hid_ref, ends.at[2])
    copies = fetch_layers(slots, 2, marks, pieces, held, sems)
    fetch.start()
    tokens, width = sum_ref.shape
    tile = next(t for t in (768, 512, 256, 128, width) if width % t == 0)
    for copy in heads:
        copy.wait()
    att = head_of(own_ref, other_ref, marks[1], marks[0])
    for _, copy in copies:
        copy.wait()
    square = jnp.zeros((tokens, 1), jnp.float32)
    for n in range(width // tile):
        part = slice(n * tile, (n + 1) * tile)
        total = early_ref[:, part] + jnp.dot(
            att, held[0, :, part], preferred_element_type=jnp.float32
        )
        sum_ref[:, part] = total
        square = square + jnp.sum(total * total, axis=1, keepdims=True)
    scale = lax.rsqrt(square / width + EPS)
    fetch.wait()
    step = 64
    stores = []
    for m in range(tokens // step):
        rows = slice(m * step, (m + 1) * step)
        branch = sum_ref[rows, :] * scale[rows] * gain_ref[...]
        out_ref[rows, :] = (hid_ref[rows, :].astype(jnp.float32) + branch).astype(jnp.bfloat16)
        stores.append(
            pltpu.make_async_copy(out_ref.at[rows, :], out_hbm.at[rows, :], ends.at[3 + m])
        )
        stores[-1].start()
    for store in stores:
        store.wait()


def out_project(own, other, arrays, slots, marks, heads, rows, finish=None):
    width = arrays[0].shape[2]
    tokens = own.shape[1]
    total = sum(len(blocks) for blocks in slots)
    vmem, left = pl.BlockSpec(memory_space=pltpu.VMEM), pl.BlockSpec(memory_space=pl.ANY)
    held = [pltpu.VMEM((heads, rows, width), jnp.bfloat16)]
    held += [pltpu.VMEM(own.shape, jnp.bfloat16)] * 2
    sems = [pltpu.SemaphoreType.DMA((total,))]
    extra, specs = [], []
    if finish:
        early, gain, hidden = finish
        extra, specs = [early, gain] + in_hbm([hidden]), [vmem, vmem, left]
        held += [
            pltpu.VMEM((tokens, width), jnp.bfloat16),
            pltpu.VMEM((tokens, width), jnp.float32),
            pltpu.VMEM((tokens, width), jnp.bfloat16),
        ]
        sems.append(pltpu.SemaphoreType.DMA((3 + tokens // 64,)))
        body = functools.partial(finish_kernel, slots)
    else:
        sems.append(pltpu.SemaphoreType.DMA((2,)))
        body = functools.partial(early_kernel, slots, heads)
    return pl.pallas_call(
        body,
        out_shape=jax.ShapeDtypeStruct((tokens, width), jnp.bfloat16 if finish else jnp.float32),
        in_specs=[pl.BlockSpec(memory_space=pltpu.SMEM)]
        + [left] * 2
        + specs
        + [left] * len(arrays),
        out_specs=left if finish else vmem,
        scratch_shapes=held + sems,
        compiler_params=pltpu.CompilerParams(vmem_limit_bytes=14 * 1024 * 1024),
        cost_estimate=pl.CostEstimate(
            flops=2 * tokens * rows * heads * width,
            bytes_accessed=2 * rows * heads * width,
            transcendentals=0,
        ),
        name="finish" if finish else "early",
    )(marks, own, other, *extra, *in_hbm(arrays))


def per_device(hidden_in, segment_ids, pre_gain, w_qkv, w_out, post_gain):
    return layer(hidden_in, segment_ids, pre_gain, w_qkv, w_out, post_gain)


def layer(hidden_in, segment_ids, pre_gain, w_qkv, w_out, post_gain):
    tok_rows, model = hidden_in.shape[1:]
    seq_count = lax.axis_size("seq")
    line_count = seq_count // 4
    seq_index = lax.axis_index("seq")
    plane = lax.axis_index("batch")
    core, pair, line = seq_index % 2, (seq_index // 2) % 2, seq_index // 4
    chip = seq_index // 2
    chip_rows = 2 * tok_rows

    half_rows = w_out.shape[0] // 2
    came = swap_core(w_qkv)
    own_kv, own_q, kv_unit, q_unit, out_unit = prepare(w_qkv, came, w_out, core, plane)
    first_pos, out_unit = lax.optimization_barrier((chip * chip_rows, out_unit))
    kv_pieces = gather_near(own_kv, kv_unit, plane, pair, line_count, "1")
    q_pieces = gather_wide(own_q, q_unit, plane, pair, line_count)
    out_own = w_out.reshape(2, half_rows, model)
    out_pieces = gather_near(out_own, out_unit, plane, pair, line_count, "3")

    cosine, sine = rotary_tables(first_pos + jnp.arange(chip_rows, dtype=jnp.int32))
    normed = norm(hidden_in[0], pre_gain, [cosine, sine], line_count)
    normed_other = swap_core(normed)
    ids = (segment_ids, swap_core(segment_ids))

    def projected(pieces, backs, **more):
        layers = [(line - back + line_count) % line_count for back in backs]
        spots, arrays, slots = [], [], []
        for block, blocks in pieces:
            if not any(back in backs for back, _, _ in blocks):
                continue
            arrays.append(block)
            slots.append(tuple(backs.index(back) for back, _, _ in blocks))
            spots += [y * 2 + h for _, y, h in blocks]
        spots = jnp.stack([jnp.asarray(spot, jnp.int32) for spot in layers + spots + [core]])
        return project(normed, normed_other, arrays, tuple(slots), len(backs), spots, **more)

    kv = projected(kv_pieces, [0, 1, 2, 3], turned=(True, False), tables=(cosine, sine), ids=ids)
    old = from_chip_behind(kv, 1)
    q = projected(q_pieces, [0, 1, 2])
    last = line_count - 1
    final = [(block, blocks) for block, blocks in q_pieces if blocks[0][0] == last]
    place = [core, chip, (line - last + line_count) % line_count]
    place += [y * 2 + h for _, blocks in final for _, y, h in blocks]
    att_own, att_send = attend(
        normed,
        normed_other,
        [block for block, _ in final],
        tuple(len(blocks) for _, blocks in final),
        jnp.stack([jnp.asarray(entry, jnp.int32) for entry in place]),
        q,
        (cosine, sine),
        kv,
        old,
        ids,
    )
    att_other = swap_core(att_send)

    swapped = [swap_core(block) for block, _ in out_pieces]

    def out_part(backs, finish=None):
        heads = [(line - back + line_count) % line_count for back in backs]
        offsets, arrays, where = [], [], []
        for (block, blocks), other in zip(out_pieces, swapped):
            if blocks[0][0] not in backs:
                continue
            for array, c in ((block, core), (other, 1 - core)):
                arrays.append(array)
                where.append(tuple(backs.index(back) for back, _, _ in blocks))
                offsets += [((y * 2 + c) * 2 + h) * half_rows for _, y, h in blocks]
        marks = jnp.stack([jnp.asarray(mark, jnp.int32) for mark in heads + [core] + offsets])
        return out_project(att_own, att_other, arrays, tuple(where), marks, len(backs), 8 * half_rows, finish)

    early = out_part([0, 1, 2])
    done = out_part([3], (early, post_gain[None, :], hidden_in[0]))
    return done[None]


BY_BATCH = ("3n",)


def from_behind(block, axis, distance):
    devices = range(lax.axis_size(axis))
    route = [(i - distance, i) for i in devices if i - distance in devices]
    return lax.ppermute(block, axis, route)


def rotary(values, positions, leading):
    head_size = values.shape[-1]
    half_dim = head_size // 2
    inverse = 1.0 / 10000.0 ** (jnp.arange(half_dim, dtype=jnp.float32) * 2.0 / head_size)
    angles = positions.astype(jnp.float32)[:, None] * inverse[None, :]
    shape = (
        (1,) * leading + (positions.shape[0],) + (1,) * (values.ndim - 2 - leading) + (half_dim,)
    )
    cosine = jnp.cos(angles).reshape(shape)
    sine = jnp.sin(angles).reshape(shape)
    first_half = values[..., :half_dim]
    second_half = values[..., half_dim:]
    return jnp.concatenate(
        [first_half * cosine - second_half * sine, second_half * cosine + first_half * sine],
        axis=-1,
    )


def attend_block(states, queries, key_block, value_block, query_pos, key_pos, starts):
    running, totals = states
    scores = jnp.einsum(
        "qhgd,khd->qhgk", queries, key_block, preferred_element_type=jnp.float32
    ) * (1.0 / math.sqrt(HEAD))
    capped = CAP * jnp.tanh(scores / CAP)
    allowed = (
        (key_pos[None, :] <= query_pos[:, None])
        & (query_pos[:, None] - key_pos[None, :] < WINDOW)
        & (key_pos[None, :] >= starts[:, None])
    )
    weights = jnp.where(allowed[:, None, None, :], jnp.exp(capped), 0.0)
    totals = totals + jnp.sum(weights, axis=-1)
    running = running + jnp.einsum(
        "qhgk,khd->qhgd",
        weights.astype(jnp.bfloat16),
        value_block,
        preferred_element_type=jnp.float32,
    )
    return (running, totals)


def per_device_general(hidden_in, segment_ids, pre_gain, w_qkv, w_out, post_gain):
    tok_rows = hidden_in.shape[1]
    seq_count = lax.axis_size("seq")
    seq_index = lax.axis_index("seq")
    groups = Q_HEADS // KV_HEADS
    positions = seq_index * tok_rows + jnp.arange(tok_rows, dtype=jnp.int32)
    widened = hidden_in[0].astype(jnp.float32)
    normed = rms_scale(widened, pre_gain).astype(jnp.bfloat16)
    columns = normed
    projected = jnp.dot(
        columns,
        lax.all_gather(w_qkv, "seq", axis=0, tiled=True),
        preferred_element_type=jnp.float32,
    )
    queries = rotary(
        projected[:, : Q_HEADS * HEAD].reshape(tok_rows, KV_HEADS, groups, HEAD), positions, 0
    ).astype(jnp.bfloat16)
    key_rows = rotary(
        projected[:, Q_HEADS * HEAD : (Q_HEADS + KV_HEADS) * HEAD].reshape(
            tok_rows, KV_HEADS, HEAD
        ),
        positions,
        0,
    ).astype(jnp.bfloat16)
    value_rows = (
        projected[:, (Q_HEADS + KV_HEADS) * HEAD :]
        .reshape(tok_rows, KV_HEADS, HEAD)
        .astype(jnp.bfloat16)
    )
    doc_numbers = jnp.arange(DOCS, dtype=jnp.int32)
    matches = segment_ids[0][:, None] == doc_numbers[None, :]
    local_first = jnp.min(jnp.where(matches, positions[:, None], seq_count * tok_rows), axis=0)
    first_pos = lax.pmin(local_first, "seq")
    starts = jnp.sum(jnp.where(matches, first_pos[None, :], 0), axis=1)
    states = (
        jnp.zeros((tok_rows, KV_HEADS, groups, HEAD), jnp.float32),
        jnp.zeros((tok_rows, KV_HEADS, groups), jnp.float32),
    )
    states = attend_block(states, queries, key_rows, value_rows, positions, positions, starts)
    longest = min(2 * seq_count * tok_rows // DOCS, WINDOW)
    hop_count = min(-(-(longest - 1) // tok_rows), seq_count - 1)

    def relay_step(hop_index, carried):
        moving_keys, moving_values, running, totals = carried
        moving_keys, moving_values = from_behind((moving_keys, moving_values), "seq", 1)
        running, totals = attend_block(
            (running, totals),
            queries,
            moving_keys,
            moving_values,
            positions,
            positions - hop_index * tok_rows,
            starts,
        )
        return (moving_keys, moving_values, running, totals)

    carried = lax.fori_loop(
        1, hop_count + 1, relay_step, (key_rows, value_rows, states[0], states[1])
    )
    states = (carried[2], carried[3])
    running, totals = states
    attended = (running / totals[..., None]).astype(jnp.bfloat16).reshape(tok_rows, Q_HEADS * HEAD)
    columns = attended
    branch = jnp.dot(
        columns,
        lax.all_gather(w_out, "seq", axis=0, tiled=True),
        preferred_element_type=jnp.float32,
    )
    return (widened + rms_scale(branch, post_gain)).astype(jnp.bfloat16)[None]


def solution(mesh):
    seq_count, planes = mesh.shape["seq"], mesh.shape["batch"]
    special = seq_count == 4 * Q_HEADS == DOCS and planes == 2 == KV_HEADS and Q_HEADS == 4
    placed = (P("batch", "seq", None), P("batch", "seq"), P(), P("seq", None), P("seq", None), P())
    return jax.shard_map(
        per_device if special else per_device_general,
        mesh=mesh,
        in_specs=placed,
        out_specs=P("batch", "seq", None),
        check_vma=False,
    )
```

```python
import functools
import math

import jax
import jax.numpy as jnp
from jax import lax
from jax.experimental import pallas as pl
from jax.experimental.pallas import tpu as pltpu
from jax.sharding import PartitionSpec as P


Q_HEADS = 4
KV_HEADS = 2
HEAD = 256
WINDOW = 4096
DOCS = 16
EPS = 1e-06
CAP = 50.0
TAIL = 16
GROUPS = Q_HEADS // KV_HEADS


def rms_scale(values, gain):
    return values * lax.rsqrt(jnp.mean(values * values, axis=-1, keepdims=True) + EPS) * gain


def rotary_tables(positions):
    half_dim = HEAD // 2
    inverse = 1.0 / 10000.0 ** (jnp.arange(half_dim, dtype=jnp.float32) * 2.0 / HEAD)
    angles = positions.astype(jnp.float32)[:, None] * inverse[None, :]
    return jnp.cos(angles), jnp.sin(angles)


def swap_core(block):
    return lax.ppermute(block, "seq", [(i, i ^ 1) for i in range(lax.axis_size("seq"))])


def swap_pair(block):
    return lax.ppermute(block, "seq", [(i, i ^ 2) for i in range(lax.axis_size("seq"))])


def swap_batch(block):
    return lax.ppermute(block, "batch", [(0, 1), (1, 0)])


def along_line(block, steps):
    count = lax.axis_size("seq")
    return lax.ppermute(block, "seq", [(i, (i + 4 * steps) % count) for i in range(count)])


def from_chip_behind(block, distance):
    count = lax.axis_size("seq")
    return lax.ppermute(block, "seq", [(i, (i + 2 * distance) % count) for i in range(count)])


def line_gather(unit, line_count):
    units = []
    for _ in range(1, line_count):
        unit = along_line(unit, 1)
        units.append(unit)
    return units


def gather_near(own, unit, plane, pair, line_count, tag):
    pair_own = swap_pair(own)
    pieces = [(own, [(0, pair, 0), (0, pair, 1)]), (pair_own, [(0, 1 - pair, 0), (0, 1 - pair, 1)])]
    first, second, third = line_gather(unit, line_count)
    near = pack(first, second[None], 0)
    for name, block, backs in (("n", near, (1, 2)), ("f", third[None], (3,))):
        pieces.append((block, [(k, pair, plane) for k in backs]))
        beside = swap_batch(block)
        pieces.append((beside, [(k, pair, 1 - plane) for k in backs]))
        across = swap_pair(block)
        pieces.append((across, [(k, 1 - pair, plane) for k in backs]))
        if tag + name in BY_BATCH:
            corner = swap_batch(across)
        else:
            corner = swap_pair(beside)
        pieces.append((corner, [(k, 1 - pair, 1 - plane) for k in backs]))
    return pieces


def gather_wide(own, mine, plane, pair, line_count):
    pair_own = swap_pair(own)
    pieces = [(own, [(0, pair, 0), (0, pair, 1)]), (pair_own, [(0, 1 - pair, 0), (0, 1 - pair, 1)])]
    unit = pack(mine, pair_own, plane)
    for back, block in enumerate(line_gather(unit, line_count), 1):
        pieces.append((block, [(back, pair, plane), (back, 1 - pair, plane)]))
        other = swap_batch(block)
        pieces.append((other, [(back, pair, 1 - plane), (back, 1 - pair, 1 - plane)]))
    return pieces


def in_hbm(arrays):
    return [pltpu.with_memory_space_constraint(array, pltpu.HBM) for array in arrays]


def pack_kernel(place, first_ref, second_ref, out_ref):
    out_ref[0] = first_ref[...]
    out_ref[1] = second_ref[place[0]]


def pack(first, second, index):
    vmem = pl.BlockSpec(memory_space=pltpu.VMEM)
    return pl.pallas_call(
        pack_kernel,
        out_shape=jax.ShapeDtypeStruct((2,) + first.shape, first.dtype),
        in_specs=[pl.BlockSpec(memory_space=pltpu.SMEM)] + [vmem] * 2,
        out_specs=vmem,
        compiler_params=pltpu.CompilerParams(vmem_limit_bytes=4 * 1024 * 1024),
        cost_estimate=pl.CostEstimate(flops=1000000, bytes_accessed=6 * first.size, transcendentals=0),
        name="pack",
    )(jnp.asarray(index, jnp.int32)[None], first, second)


def prepare_kernel(place, w_ref, came_ref, out_ref, kv_ref, q_ref, kv_unit, q_unit, out_unit):
    core, plane = place[0], place[1]
    rows = out_ref.shape[0] // 2
    at_q = pl.multiple_of(core * GROUPS * HEAD, 128)
    at_k = pl.multiple_of((Q_HEADS + core) * HEAD, 128)
    at_v = pl.multiple_of((Q_HEADS + KV_HEADS + core) * HEAD, 128)
    out_unit[...] = out_ref[pl.ds(pl.multiple_of(plane * rows, rows), rows), :]
    for ref, half in ((w_ref, core), (came_ref, 1 - core)):
        for target, low, at, width in (
            (kv_ref, 0, at_k, HEAD),
            (kv_ref, HEAD, at_v, HEAD),
            (q_ref, 0, at_q, GROUPS * HEAD),
        ):
            block = ref[:, pl.ds(at, width)]
            target[half, :, low : low + width] = block
            unit = kv_unit if target is kv_ref else q_unit

            @pl.when(half == plane)
            def _():
                unit[:, low : low + width] = block


def prepare(w_qkv, came, w_out, core, plane):
    rows = w_qkv.shape[0]
    vmem = pl.BlockSpec(memory_space=pltpu.VMEM)
    kv, q = 2 * HEAD, GROUPS * HEAD
    return pl.pallas_call(
        prepare_kernel,
        out_shape=[
            jax.ShapeDtypeStruct(shape, jnp.bfloat16)
            for shape in (
                (2, rows, kv),
                (2, rows, q),
                (rows, kv),
                (rows, q),
                (w_out.shape[0] // 2, w_out.shape[1]),
            )
        ],
        in_specs=[pl.BlockSpec(memory_space=pltpu.SMEM)] + [vmem] * 3,
        out_specs=[vmem] * 5,
        compiler_params=pltpu.CompilerParams(vmem_limit_bytes=12 * 1024 * 1024),
        cost_estimate=pl.CostEstimate(flops=1000000, bytes_accessed=2 * w_qkv.size, transcendentals=0),
        name="prepare",
    )(jnp.stack([core, plane]).astype(jnp.int32), *in_hbm([w_qkv]), came, *in_hbm([w_out]))


def norm_kernel(in_ref, gain_ref, cos_ref, sin_ref, out_ref):
    step = 64

    def body(i, carry):
        at = pl.ds(pl.multiple_of(i * step, step), step)
        normed = rms_scale(in_ref[at, :].astype(jnp.float32), gain_ref[...]).astype(jnp.bfloat16)
        depth = normed.shape[1] // out_ref.shape[0]
        for part in range(out_ref.shape[0]):
            out_ref[part, at, :depth] = normed[:, part * depth : (part + 1) * depth]
        return carry

    lax.fori_loop(0, in_ref.shape[0] // step, body, 0)


def norm(rows, gain, tables, parts):
    count, width = rows.shape
    vmem = pl.BlockSpec(memory_space=pltpu.VMEM)
    return pl.pallas_call(
        norm_kernel,
        out_shape=jax.ShapeDtypeStruct((parts, count, -(-width // parts // 128) * 128), jnp.bfloat16),
        in_specs=[vmem] * 2 + [pl.BlockSpec(memory_space=pl.ANY)] * 2,
        out_specs=vmem,
        compiler_params=pltpu.CompilerParams(vmem_limit_bytes=8 * 1024 * 1024),
        cost_estimate=pl.CostEstimate(flops=1000000, bytes_accessed=4 * rows.size, transcendentals=0),
        name="norm",
    )(*in_hbm([rows]), gain[None, :], *in_hbm(tables))


def fetch_layers(slots, first, marks, pieces, held, sems):
    rows = pieces[0].shape[1]
    copies = []
    for piece, blocks in zip(pieces, slots):
        for i, slot in enumerate(blocks):
            at = pl.multiple_of(marks[first + len(copies)], rows)
            copy = pltpu.make_async_copy(
                piece.at[i], held.at[slot, pl.ds(at, rows), :], sems.at[len(copies)]
            )
            copy.start()
            copies.append((slot, copy))
    return copies


def fetch_pair(first_hbm, second_hbm, first_ref, second_ref, sems):
    copies = (
        pltpu.make_async_copy(first_hbm, first_ref, sems.at[0]),
        pltpu.make_async_copy(second_hbm, second_ref, sems.at[1]),
    )
    for copy in copies:
        copy.start()
    return copies


def project_kernel(slots, turned, spots, x_ref, other_ref, cos_hbm, sin_hbm, ids_ref, other_ids_ref, *refs):
    pieces = refs[: len(slots)]
    out_ref, held, total, cos_ref, sin_ref, sems, ends = refs[len(slots) :]
    layers = held.shape[0]
    copies = fetch_layers(slots, layers, spots, pieces, held, sems)
    tables = fetch_pair(cos_hbm, sin_hbm, cos_ref, sin_ref, ends)
    core = spots[layers + len(copies)]
    tokens = x_ref.shape[1]
    mine = pl.ds(pl.multiple_of(core * tokens, tokens), tokens)
    theirs = pl.ds(pl.multiple_of((1 - core) * tokens, tokens), tokens)
    for ref, at in ((ids_ref, mine), (other_ids_ref, theirs)):
        row = jnp.broadcast_to(ref[...].astype(jnp.float32), (TAIL, tokens))
        out_ref[2 * tokens :, at] = row.astype(jnp.bfloat16)
    half = HEAD // 2
    for layer in range(layers):
        for slot, copy in copies:
            if slot == layer:
                copy.wait()
        last = layer == layers - 1
        if last:
            for copy in tables:
                copy.wait()
        for ref, at in ((x_ref, mine), (other_ref, theirs)):
            part = jnp.dot(
                ref[spots[layer], :, : held.shape[1]], held[layer], preferred_element_type=jnp.float32
            )
            if layer > 0:
                part = part + total[at, :]
            if not last:
                total[at, :] = part
                continue
            cosine, sine = cos_ref[at, :], sin_ref[at, :]
            for h, turn in enumerate(turned):
                a = part[:, h * HEAD : h * HEAD + half]
                b = part[:, h * HEAD + half : (h + 1) * HEAD]
                if turn:
                    a, b = a * cosine - b * sine, b * cosine + a * sine
                out_ref[at, h * HEAD : h * HEAD + half] = a.astype(jnp.bfloat16)
                out_ref[at, h * HEAD + half : (h + 1) * HEAD] = b.astype(jnp.bfloat16)


def project(x, other, arrays, slots, layers, spots, turned, tables, ids):
    tokens, depth, width = 2 * x.shape[1], 4 * arrays[0].shape[1], arrays[0].shape[2]
    vmem, left = pl.BlockSpec(memory_space=pltpu.VMEM), pl.BlockSpec(memory_space=pl.ANY)
    return pl.pallas_call(
        functools.partial(project_kernel, slots, turned),
        out_shape=jax.ShapeDtypeStruct((tokens + TAIL, width), jnp.bfloat16),
        in_specs=[pl.BlockSpec(memory_space=pltpu.SMEM)]
        + [vmem, vmem, left, left, vmem, vmem]
        + [left] * len(arrays),
        out_specs=vmem,
        scratch_shapes=[
            pltpu.VMEM((layers, depth, width), jnp.bfloat16),
            pltpu.VMEM((tokens, width), jnp.float32),
            pltpu.VMEM((tokens, HEAD // 2), jnp.float32),
            pltpu.VMEM((tokens, HEAD // 2), jnp.float32),
            pltpu.SemaphoreType.DMA((sum(len(blocks) for blocks in slots),)),
            pltpu.SemaphoreType.DMA((2,)),
        ],
        compiler_params=pltpu.CompilerParams(vmem_limit_bytes=12 * 1024 * 1024),
        cost_estimate=pl.CostEstimate(
            flops=2 * tokens * depth * layers * width,
            bytes_accessed=2 * layers * depth * width,
            transcendentals=0,
        ),
        name="project",
    )(spots, x, other, *in_hbm(tables), *ids, *in_hbm(arrays))


def attend_kernel(slots, layers, place, x_ref, other_ref, ids_ref, *refs):
    other_ids_ref, cos_hbm, sin_hbm, kv_hbm, old_hbm = refs[:5]
    pieces, refs = refs[5 : 5 + len(slots)], refs[5 + len(slots) :]
    own_ref, send_ref, held, total, q_ref, cos_ref, sin_ref, kv_ref, old_ref, sems, turns, ends = refs
    copies = fetch_layers(slots, 2 + layers, place, pieces, held, sems)
    tables = fetch_pair(cos_hbm, sin_hbm, cos_ref, sin_ref, turns)
    fetch = fetch_pair(kv_hbm, old_hbm, kv_ref, old_ref, ends)
    core, chip = place[0], place[1]
    step = own_ref.shape[1]
    tokens = q_ref.shape[0]
    behind = tokens
    first = core == 0
    ids = jnp.concatenate(
        [
            jnp.where(first, ids_ref[...], other_ids_ref[...]),
            jnp.where(first, other_ids_ref[...], ids_ref[...]),
        ],
        axis=1,
    ).astype(jnp.float32)
    query_ids = jnp.broadcast_to(ids, (128, tokens)).T[:, :1]
    half = HEAD // 2
    for layer in range(layers):
        for slot, copy in copies:
            if slot == layer:
                copy.wait()
        for ref, block in ((x_ref, 0), (other_ref, 1)):
            part = jnp.dot(
                ref[place[2 + layer], :, : held.shape[1]],
                held[layer],
                preferred_element_type=jnp.float32,
            )
            total[block] = part if layer == 0 else total[block] + part
    for copy in tables:
        copy.wait()
    for block, at in ((0, core), (1, 1 - core)):
        part = total[block]
        at = pl.ds(pl.multiple_of(at * step, step), step)
        cosine, sine = cos_ref[at, :], sin_ref[at, :]
        for h in range(GROUPS):
            a = part[:, h * HEAD : h * HEAD + half]
            b = part[:, h * HEAD + half : (h + 1) * HEAD]
            q_ref[at, h * HEAD : h * HEAD + half] = (a * cosine - b * sine).astype(jnp.bfloat16)
            q_ref[at, h * HEAD + half : (h + 1) * HEAD] = (b * cosine + a * sine).astype(
                jnp.bfloat16
            )
    for copy in fetch:
        copy.wait()
    old_ids = old_ref[behind : behind + TAIL, :].astype(jnp.float32)[:1]
    key_ids = jnp.concatenate([jnp.where(chip > 0, old_ids, -1.0), ids], axis=1)
    for m in range(tokens // step):
        low = m * step
        top = behind + (m + 1) * step
        span = top - low
        qpos = behind + m * step + lax.broadcasted_iota(jnp.int32, (step, span), 0)
        kpos = low + lax.broadcasted_iota(jnp.int32, (step, span), 1)
        same = query_ids[m * step : (m + 1) * step, :] == key_ids[:, low:top]
        allowed = same & (kpos <= qpos) & (qpos - kpos < WINDOW)
        keys = jnp.concatenate([old_ref[low:behind, :HEAD], kv_ref[: (m + 1) * step, :HEAD]], axis=0)
        values = jnp.concatenate(
            [old_ref[low:behind, HEAD:], kv_ref[: (m + 1) * step, HEAD:]], axis=0
        )
        for h in range(GROUPS):
            q = q_ref[m * step : (m + 1) * step, h * HEAD : (h + 1) * HEAD]
            scores = lax.dot_general(
                q, keys, (((1,), (1,)), ((), ())), preferred_element_type=jnp.float32
            )
            capped = CAP * jnp.tanh(scores * (1.0 / (CAP * math.sqrt(HEAD))))
            weights = jnp.where(allowed, jnp.exp(capped), 0.0)
            totals = jnp.sum(weights, axis=1, keepdims=True)
            mixed = jnp.dot(
                weights.astype(jnp.bfloat16), values, preferred_element_type=jnp.float32
            )
            result = (mixed / totals).astype(jnp.bfloat16)

            @pl.when(core == m)
            def _():
                own_ref[h] = result

            @pl.when(core != m)
            def _():
                send_ref[h] = result


def attend(x, other, arrays, slots, layers, place, tables, kv, old, ids):
    tokens, depth, width = 2 * x.shape[1], 4 * arrays[0].shape[1], arrays[0].shape[2]
    work = GROUPS * tokens * 2 * tokens * HEAD
    vmem, left = pl.BlockSpec(memory_space=pltpu.VMEM), pl.BlockSpec(memory_space=pl.ANY)
    return pl.pallas_call(
        functools.partial(attend_kernel, slots, layers),
        out_shape=[jax.ShapeDtypeStruct((GROUPS, tokens // 2, HEAD), jnp.bfloat16)] * 2,
        in_specs=[pl.BlockSpec(memory_space=pltpu.SMEM)] + [vmem] * 4 + [left] * (4 + len(arrays)),
        out_specs=[vmem] * 2,
        scratch_shapes=[
            pltpu.VMEM((layers, depth, width), jnp.bfloat16),
            pltpu.VMEM((2, tokens // 2, width), jnp.float32),
            pltpu.VMEM((tokens, width), jnp.bfloat16),
            pltpu.VMEM((tokens, HEAD // 2), jnp.float32),
            pltpu.VMEM((tokens, HEAD // 2), jnp.float32),
            pltpu.VMEM(kv.shape, jnp.bfloat16),
            pltpu.VMEM(old.shape, jnp.bfloat16),
            pltpu.SemaphoreType.DMA((sum(len(blocks) for blocks in slots),)),
            pltpu.SemaphoreType.DMA((2,)),
            pltpu.SemaphoreType.DMA((2,)),
        ],
        compiler_params=pltpu.CompilerParams(vmem_limit_bytes=20 * 1024 * 1024),
        cost_estimate=pl.CostEstimate(
            flops=4 * work, bytes_accessed=work // 256, transcendentals=0
        ),
        name="attend",
    )(place, x, other, *ids, *in_hbm(tables), *in_hbm([kv, old]), *in_hbm(arrays))


def head_of(own_ref, other_ref, core, head):
    return jnp.where(head // GROUPS == core, own_ref[head % GROUPS], other_ref[head % GROUPS])


def early_kernel(slots, heads, marks, own_hbm, other_hbm, *refs):
    pieces = refs[: len(slots)]
    out_ref, held, own_ref, other_ref, sems, ends = refs[len(slots) :]
    fetch = fetch_pair(own_hbm, other_hbm, own_ref, other_ref, ends)
    copies = fetch_layers(slots, heads + 1, marks, pieces, held, sems)
    for copy in fetch:
        copy.wait()
    width = out_ref.shape[1]
    tile = next(t for t in (768, 512, 256, 128, width) if width % t == 0)
    for s in range(heads):
        for slot, copy in copies:
            if slot == s:
                copy.wait()
        att = head_of(own_ref, other_ref, marks[heads], marks[s])
        for n in range(width // tile):
            part = slice(n * tile, (n + 1) * tile)
            product = jnp.dot(att, held[s, :, part], preferred_element_type=jnp.float32)
            out_ref[:, part] = product if s == 0 else out_ref[:, part] + product


def finish_kernel(slots, marks, own_hbm, other_hbm, early_ref, gain_ref, hid_hbm, *refs):
    pieces = refs[: len(slots)]
    out_hbm, held, own_ref, other_ref, hid_ref, sum_ref, out_ref, sems, ends = refs[len(slots) :]
    heads = fetch_pair(own_hbm, other_hbm, own_ref, other_ref, ends)
    fetch = pltpu.make_async_copy(hid_hbm, hid_ref, ends.at[2])
    copies = fetch_layers(slots, 2, marks, pieces, held, sems)
    fetch.start()
    tokens, width = sum_ref.shape
    tile = next(t for t in (768, 512, 256, 128, width) if width % t == 0)
    for copy in heads:
        copy.wait()
    att = head_of(own_ref, other_ref, marks[1], marks[0])
    for _, copy in copies:
        copy.wait()
    square = jnp.zeros((tokens, 1), jnp.float32)
    for n in range(width // tile):
        part = slice(n * tile, (n + 1) * tile)
        total = early_ref[:, part] + jnp.dot(
            att, held[0, :, part], preferred_element_type=jnp.float32
        )
        sum_ref[:, part] = total
        square = square + jnp.sum(total * total, axis=1, keepdims=True)
    scale = lax.rsqrt(square / width + EPS)
    fetch.wait()
    step = 64
    stores = []
    for m in range(tokens // step):
        rows = slice(m * step, (m + 1) * step)
        branch = sum_ref[rows, :] * scale[rows] * gain_ref[...]
        out_ref[rows, :] = (hid_ref[rows, :].astype(jnp.float32) + branch).astype(jnp.bfloat16)
        stores.append(
            pltpu.make_async_copy(out_ref.at[rows, :], out_hbm.at[rows, :], ends.at[3 + m])
        )
        stores[-1].start()
    for store in stores:
        store.wait()


def out_project(own, other, arrays, slots, marks, heads, rows, finish=None):
    width = arrays[0].shape[2]
    tokens = own.shape[1]
    total = sum(len(blocks) for blocks in slots)
    vmem, left = pl.BlockSpec(memory_space=pltpu.VMEM), pl.BlockSpec(memory_space=pl.ANY)
    held = [pltpu.VMEM((heads, rows, width), jnp.bfloat16)]
    held += [pltpu.VMEM(own.shape, jnp.bfloat16)] * 2
    sems = [pltpu.SemaphoreType.DMA((total,))]
    extra, specs = [], []
    if finish:
        early, gain, hidden = finish
        extra, specs = [early, gain] + in_hbm([hidden]), [vmem, vmem, left]
        held += [
            pltpu.VMEM((tokens, width), jnp.bfloat16),
            pltpu.VMEM((tokens, width), jnp.float32),
            pltpu.VMEM((tokens, width), jnp.bfloat16),
        ]
        sems.append(pltpu.SemaphoreType.DMA((3 + tokens // 64,)))
        body = functools.partial(finish_kernel, slots)
    else:
        sems.append(pltpu.SemaphoreType.DMA((2,)))
        body = functools.partial(early_kernel, slots, heads)
    return pl.pallas_call(
        body,
        out_shape=jax.ShapeDtypeStruct((tokens, width), jnp.bfloat16 if finish else jnp.float32),
        in_specs=[pl.BlockSpec(memory_space=pltpu.SMEM)]
        + [left] * 2
        + specs
        + [left] * len(arrays),
        out_specs=left if finish else vmem,
        scratch_shapes=held + sems,
        compiler_params=pltpu.CompilerParams(vmem_limit_bytes=14 * 1024 * 1024),
        cost_estimate=pl.CostEstimate(
            flops=2 * tokens * rows * heads * width,
            bytes_accessed=2 * rows * heads * width,
            transcendentals=0,
        ),
        name="finish" if finish else "early",
    )(marks, own, other, *extra, *arrays)


def per_device(hidden_in, segment_ids, pre_gain, w_qkv, w_out, post_gain):
    return layer(hidden_in, segment_ids, pre_gain, w_qkv, w_out, post_gain)


def layer(hidden_in, segment_ids, pre_gain, w_qkv, w_out, post_gain):
    tok_rows, model = hidden_in.shape[1:]
    seq_count = lax.axis_size("seq")
    line_count = seq_count // 4
    seq_index = lax.axis_index("seq")
    plane = lax.axis_index("batch")
    core, pair, line = seq_index % 2, (seq_index // 2) % 2, seq_index // 4
    chip = seq_index // 2
    chip_rows = 2 * tok_rows

    half_rows = w_out.shape[0] // 2
    came = swap_core(w_qkv)
    own_kv, own_q, kv_unit, q_unit, out_unit = prepare(w_qkv, came, w_out, core, plane)
    first_pos, out_unit = lax.optimization_barrier((chip * chip_rows, out_unit))
    kv_pieces = gather_near(own_kv, kv_unit, plane, pair, line_count, "1")
    q_pieces = gather_wide(own_q, q_unit, plane, pair, line_count)
    out_own = w_out.reshape(2, half_rows, model)
    out_pieces = gather_near(out_own, out_unit, plane, pair, line_count, "3")

    cosine, sine = rotary_tables(first_pos + jnp.arange(chip_rows, dtype=jnp.int32))
    normed = norm(hidden_in[0], pre_gain, [cosine, sine], line_count)
    normed_other = swap_core(normed)
    ids = (segment_ids, swap_core(segment_ids))

    backs = list(range(line_count))
    layers = [(line - back + line_count) % line_count for back in backs]

    def laid(pieces):
        arrays = [block for block, _ in pieces]
        slots = tuple(tuple(back for back, _, _ in blocks) for _, blocks in pieces)
        rows = arrays[0].shape[1]
        return arrays, slots, [(y * 2 + h) * rows for _, blocks in pieces for _, y, h in blocks]

    def scalars(entries):
        return jnp.stack([jnp.asarray(entry, jnp.int32) for entry in entries])

    arrays, slots, spots = laid(kv_pieces)
    kv = project(
        normed,
        normed_other,
        arrays,
        slots,
        line_count,
        scalars(layers + spots + [core]),
        turned=(True, False),
        tables=(cosine, sine),
        ids=ids,
    )
    old = from_chip_behind(kv, 1)
    arrays, slots, spots = laid(q_pieces)
    att_own, att_send = attend(
        normed,
        normed_other,
        arrays,
        slots,
        line_count,
        scalars([core, chip] + layers + spots),
        (cosine, sine),
        kv,
        old,
        ids,
    )
    att_other = swap_core(att_send)

    swapped = [swap_core(block) for block, _ in out_pieces]

    def out_part(backs, finish=None):
        heads = [(line - back + line_count) % line_count for back in backs]
        offsets, arrays, where = [], [], []
        for (block, blocks), other in zip(out_pieces, swapped):
            if blocks[0][0] not in backs:
                continue
            for array, c in ((in_hbm([block])[0], core), (other, 1 - core)):
                arrays.append(array)
                where.append(tuple(backs.index(back) for back, _, _ in blocks))
                offsets += [((y * 2 + c) * 2 + h) * half_rows for _, y, h in blocks]
        marks = jnp.stack([jnp.asarray(mark, jnp.int32) for mark in heads + [core] + offsets])
        return out_project(att_own, att_other, arrays, tuple(where), marks, len(backs), 8 * half_rows, finish)

    early = out_part([0, 1, 2])
    done = out_part([3], (early, post_gain[None, :], hidden_in[0]))
    return done[None]


BY_BATCH = ()


def from_behind(block, axis, distance):
    devices = range(lax.axis_size(axis))
    route = [(i - distance, i) for i in devices if i - distance in devices]
    return lax.ppermute(block, axis, route)


def rotary(values, positions, leading):
    head_size = values.shape[-1]
    half_dim = head_size // 2
    inverse = 1.0 / 10000.0 ** (jnp.arange(half_dim, dtype=jnp.float32) * 2.0 / head_size)
    angles = positions.astype(jnp.float32)[:, None] * inverse[None, :]
    shape = (
        (1,) * leading + (positions.shape[0],) + (1,) * (values.ndim - 2 - leading) + (half_dim,)
    )
    cosine = jnp.cos(angles).reshape(shape)
    sine = jnp.sin(angles).reshape(shape)
    first_half = values[..., :half_dim]
    second_half = values[..., half_dim:]
    return jnp.concatenate(
        [first_half * cosine - second_half * sine, second_half * cosine + first_half * sine],
        axis=-1,
    )


def attend_block(states, queries, key_block, value_block, query_pos, key_pos, starts):
    running, totals = states
    scores = jnp.einsum(
        "qhgd,khd->qhgk", queries, key_block, preferred_element_type=jnp.float32
    ) * (1.0 / math.sqrt(HEAD))
    capped = CAP * jnp.tanh(scores / CAP)
    allowed = (
        (key_pos[None, :] <= query_pos[:, None])
        & (query_pos[:, None] - key_pos[None, :] < WINDOW)
        & (key_pos[None, :] >= starts[:, None])
    )
    weights = jnp.where(allowed[:, None, None, :], jnp.exp(capped), 0.0)
    totals = totals + jnp.sum(weights, axis=-1)
    running = running + jnp.einsum(
        "qhgk,khd->qhgd",
        weights.astype(jnp.bfloat16),
        value_block,
        preferred_element_type=jnp.float32,
    )
    return (running, totals)


def per_device_general(hidden_in, segment_ids, pre_gain, w_qkv, w_out, post_gain):
    tok_rows = hidden_in.shape[1]
    seq_count = lax.axis_size("seq")
    seq_index = lax.axis_index("seq")
    groups = Q_HEADS // KV_HEADS
    positions = seq_index * tok_rows + jnp.arange(tok_rows, dtype=jnp.int32)
    widened = hidden_in[0].astype(jnp.float32)
    normed = rms_scale(widened, pre_gain).astype(jnp.bfloat16)
    columns = normed
    projected = jnp.dot(
        columns,
        lax.all_gather(w_qkv, "seq", axis=0, tiled=True),
        preferred_element_type=jnp.float32,
    )
    queries = rotary(
        projected[:, : Q_HEADS * HEAD].reshape(tok_rows, KV_HEADS, groups, HEAD), positions, 0
    ).astype(jnp.bfloat16)
    key_rows = rotary(
        projected[:, Q_HEADS * HEAD : (Q_HEADS + KV_HEADS) * HEAD].reshape(
            tok_rows, KV_HEADS, HEAD
        ),
        positions,
        0,
    ).astype(jnp.bfloat16)
    value_rows = (
        projected[:, (Q_HEADS + KV_HEADS) * HEAD :]
        .reshape(tok_rows, KV_HEADS, HEAD)
        .astype(jnp.bfloat16)
    )
    doc_numbers = jnp.arange(DOCS, dtype=jnp.int32)
    matches = segment_ids[0][:, None] == doc_numbers[None, :]
    local_first = jnp.min(jnp.where(matches, positions[:, None], seq_count * tok_rows), axis=0)
    first_pos = lax.pmin(local_first, "seq")
    starts = jnp.sum(jnp.where(matches, first_pos[None, :], 0), axis=1)
    states = (
        jnp.zeros((tok_rows, KV_HEADS, groups, HEAD), jnp.float32),
        jnp.zeros((tok_rows, KV_HEADS, groups), jnp.float32),
    )
    states = attend_block(states, queries, key_rows, value_rows, positions, positions, starts)
    longest = min(2 * seq_count * tok_rows // DOCS, WINDOW)
    hop_count = min(-(-(longest - 1) // tok_rows), seq_count - 1)

    def relay_step(hop_index, carried):
        moving_keys, moving_values, running, totals = carried
        moving_keys, moving_values = from_behind((moving_keys, moving_values), "seq", 1)
        running, totals = attend_block(
            (running, totals),
            queries,
            moving_keys,
            moving_values,
            positions,
            positions - hop_index * tok_rows,
            starts,
        )
        return (moving_keys, moving_values, running, totals)

    carried = lax.fori_loop(
        1, hop_count + 1, relay_step, (key_rows, value_rows, states[0], states[1])
    )
    states = (carried[2], carried[3])
    running, totals = states
    attended = (running / totals[..., None]).astype(jnp.bfloat16).reshape(tok_rows, Q_HEADS * HEAD)
    columns = attended
    branch = jnp.dot(
        columns,
        lax.all_gather(w_out, "seq", axis=0, tiled=True),
        preferred_element_type=jnp.float32,
    )
    return (widened + rms_scale(branch, post_gain)).astype(jnp.bfloat16)[None]


def solution(mesh):
    seq_count, planes = mesh.shape["seq"], mesh.shape["batch"]
    special = seq_count == 4 * Q_HEADS == DOCS and planes == 2 == KV_HEADS and Q_HEADS == 4
    placed = (P("batch", "seq", None), P("batch", "seq"), P(), P("seq", None), P("seq", None), P())
    return jax.shard_map(
        per_device if special else per_device_general,
        mesh=mesh,
        in_specs=placed,
        out_specs=P("batch", "seq", None),
        check_vma=False,
    )
```

```python
import functools
import math

import jax
import jax.numpy as jnp
from jax import lax
from jax.experimental import pallas as pl
from jax.experimental.pallas import tpu as pltpu
from jax.sharding import PartitionSpec as P


Q_HEADS = 4
KV_HEADS = 2
HEAD = 256
WINDOW = 4096
DOCS = 16
EPS = 1e-06
CAP = 50.0
TAIL = 16
GROUPS = Q_HEADS // KV_HEADS


def rms_scale(values, gain):
    return values * lax.rsqrt(jnp.mean(values * values, axis=-1, keepdims=True) + EPS) * gain


def rotary_tables(positions):
    half_dim = HEAD // 2
    inverse = 1.0 / 10000.0 ** (jnp.arange(half_dim, dtype=jnp.float32) * 2.0 / HEAD)
    angles = positions.astype(jnp.float32)[:, None] * inverse[None, :]
    return jnp.cos(angles), jnp.sin(angles)


def swap_core(block):
    return lax.ppermute(block, "seq", [(i, i ^ 1) for i in range(lax.axis_size("seq"))])


def swap_pair(block):
    return lax.ppermute(block, "seq", [(i, i ^ 2) for i in range(lax.axis_size("seq"))])


def swap_batch(block):
    return lax.ppermute(block, "batch", [(0, 1), (1, 0)])


def along_line(block, steps):
    count = lax.axis_size("seq")
    return lax.ppermute(block, "seq", [(i, (i + 4 * steps) % count) for i in range(count)])


def from_chip_behind(block, distance):
    count = lax.axis_size("seq")
    return lax.ppermute(block, "seq", [(i, (i + 2 * distance) % count) for i in range(count)])


def line_gather(unit, line_count):
    units = []
    for _ in range(1, line_count):
        unit = along_line(unit, 1)
        units.append(unit)
    return units


def gather_near(own, unit, plane, pair, line_count, tag):
    pair_own = swap_pair(own)
    pieces = [(own, [(0, pair, 0), (0, pair, 1)]), (pair_own, [(0, 1 - pair, 0), (0, 1 - pair, 1)])]
    first, second, third = line_gather(unit, line_count)
    near = pack(first, second[None], 0)
    for name, block, backs in (("n", near, (1, 2)), ("f", third[None], (3,))):
        pieces.append((block, [(k, pair, plane) for k in backs]))
        beside = swap_batch(block)
        pieces.append((beside, [(k, pair, 1 - plane) for k in backs]))
        across = swap_pair(block)
        pieces.append((across, [(k, 1 - pair, plane) for k in backs]))
        if tag + name in BY_BATCH:
            corner = swap_batch(across)
        else:
            corner = swap_pair(beside)
        pieces.append((corner, [(k, 1 - pair, 1 - plane) for k in backs]))
    return pieces


def gather_wide(own, mine, plane, pair, line_count):
    pair_own = swap_pair(own)
    pieces = [(own, [(0, pair, 0), (0, pair, 1)]), (pair_own, [(0, 1 - pair, 0), (0, 1 - pair, 1)])]
    unit = pack(mine, pair_own, plane)
    for back, block in enumerate(line_gather(unit, line_count), 1):
        pieces.append((block, [(back, pair, plane), (back, 1 - pair, plane)]))
        other = swap_batch(block)
        pieces.append((other, [(back, pair, 1 - plane), (back, 1 - pair, 1 - plane)]))
    return pieces


def in_hbm(arrays):
    return [pltpu.with_memory_space_constraint(array, pltpu.HBM) for array in arrays]


def pack_kernel(place, first_ref, second_ref, out_ref):
    out_ref[0] = first_ref[...]
    out_ref[1] = second_ref[place[0]]


def pack(first, second, index):
    vmem = pl.BlockSpec(memory_space=pltpu.VMEM)
    return pl.pallas_call(
        pack_kernel,
        out_shape=jax.ShapeDtypeStruct((2,) + first.shape, first.dtype),
        in_specs=[pl.BlockSpec(memory_space=pltpu.SMEM)] + [vmem] * 2,
        out_specs=vmem,
        compiler_params=pltpu.CompilerParams(vmem_limit_bytes=4 * 1024 * 1024),
        cost_estimate=pl.CostEstimate(flops=1000000, bytes_accessed=6 * first.size, transcendentals=0),
        name="pack",
    )(jnp.asarray(index, jnp.int32)[None], first, second)


def prepare_kernel(place, w_ref, came_ref, out_ref, kv_ref, q_ref, kv_unit, q_unit, out_unit):
    core, plane = place[0], place[1]
    rows = out_ref.shape[0] // 2
    at_q = pl.multiple_of(core * GROUPS * HEAD, 128)
    at_k = pl.multiple_of((Q_HEADS + core) * HEAD, 128)
    at_v = pl.multiple_of((Q_HEADS + KV_HEADS + core) * HEAD, 128)
    out_unit[...] = out_ref[pl.ds(pl.multiple_of(plane * rows, rows), rows), :]
    for ref, half in ((w_ref, core), (came_ref, 1 - core)):
        for target, low, at, width in (
            (kv_ref, 0, at_k, HEAD),
            (kv_ref, HEAD, at_v, HEAD),
            (q_ref, 0, at_q, GROUPS * HEAD),
        ):
            block = ref[:, pl.ds(at, width)]
            target[half, :, low : low + width] = block
            unit = kv_unit if target is kv_ref else q_unit

            @pl.when(half == plane)
            def _():
                unit[:, low : low + width] = block


def prepare(w_qkv, came, w_out, core, plane):
    rows = w_qkv.shape[0]
    vmem = pl.BlockSpec(memory_space=pltpu.VMEM)
    kv, q = 2 * HEAD, GROUPS * HEAD
    return pl.pallas_call(
        prepare_kernel,
        out_shape=[
            jax.ShapeDtypeStruct(shape, jnp.bfloat16)
            for shape in (
                (2, rows, kv),
                (2, rows, q),
                (rows, kv),
                (rows, q),
                (w_out.shape[0] // 2, w_out.shape[1]),
            )
        ],
        in_specs=[pl.BlockSpec(memory_space=pltpu.SMEM)] + [vmem] * 3,
        out_specs=[vmem] * 5,
        compiler_params=pltpu.CompilerParams(vmem_limit_bytes=12 * 1024 * 1024),
        cost_estimate=pl.CostEstimate(flops=1000000, bytes_accessed=2 * w_qkv.size, transcendentals=0),
        name="prepare",
    )(jnp.stack([core, plane]).astype(jnp.int32), *in_hbm([w_qkv]), came, *in_hbm([w_out]))


def norm_kernel(in_ref, gain_ref, cos_ref, sin_ref, out_ref):
    step = 64

    def body(i, carry):
        at = pl.ds(pl.multiple_of(i * step, step), step)
        normed = rms_scale(in_ref[at, :].astype(jnp.float32), gain_ref[...]).astype(jnp.bfloat16)
        depth = normed.shape[1] // out_ref.shape[0]
        for part in range(out_ref.shape[0]):
            out_ref[part, at, :depth] = normed[:, part * depth : (part + 1) * depth]
        return carry

    lax.fori_loop(0, in_ref.shape[0] // step, body, 0)


def norm(rows, gain, tables, parts):
    count, width = rows.shape
    vmem = pl.BlockSpec(memory_space=pltpu.VMEM)
    return pl.pallas_call(
        norm_kernel,
        out_shape=jax.ShapeDtypeStruct((parts, count, -(-width // parts // 128) * 128), jnp.bfloat16),
        in_specs=[vmem] * 2 + [pl.BlockSpec(memory_space=pl.ANY)] * 2,
        out_specs=vmem,
        compiler_params=pltpu.CompilerParams(vmem_limit_bytes=8 * 1024 * 1024),
        cost_estimate=pl.CostEstimate(flops=1000000, bytes_accessed=4 * rows.size, transcendentals=0),
        name="norm",
    )(*in_hbm([rows]), gain[None, :], *in_hbm(tables))


def fetch_layers(slots, first, marks, pieces, held, sems):
    rows = pieces[0].shape[1]
    copies = []
    for piece, blocks in zip(pieces, slots):
        for i, slot in enumerate(blocks):
            at = pl.multiple_of(marks[first + len(copies)], rows)
            copy = pltpu.make_async_copy(
                piece.at[i], held.at[slot, pl.ds(at, rows), :], sems.at[len(copies)]
            )
            copy.start()
            copies.append((slot, copy))
    return copies


def fetch_pair(first_hbm, second_hbm, first_ref, second_ref, sems):
    copies = (
        pltpu.make_async_copy(first_hbm, first_ref, sems.at[0]),
        pltpu.make_async_copy(second_hbm, second_ref, sems.at[1]),
    )
    for copy in copies:
        copy.start()
    return copies


def project_kernel(slots, turned, spots, x_ref, other_ref, cos_hbm, sin_hbm, ids_ref, other_ids_ref, *refs):
    pieces = refs[: len(slots)]
    out_ref, held, total, cos_ref, sin_ref, sems, ends = refs[len(slots) :]
    layers = held.shape[0]
    copies = fetch_layers(slots, layers, spots, pieces, held, sems)
    tables = fetch_pair(cos_hbm, sin_hbm, cos_ref, sin_ref, ends)
    core = spots[layers + len(copies)]
    tokens = x_ref.shape[1]
    mine = pl.ds(pl.multiple_of(core * tokens, tokens), tokens)
    theirs = pl.ds(pl.multiple_of((1 - core) * tokens, tokens), tokens)
    for ref, at in ((ids_ref, mine), (other_ids_ref, theirs)):
        row = jnp.broadcast_to(ref[...].astype(jnp.float32), (TAIL, tokens))
        out_ref[2 * tokens :, at] = row.astype(jnp.bfloat16)
    half = HEAD // 2
    for layer in range(layers):
        for slot, copy in copies:
            if slot == layer:
                copy.wait()
        last = layer == layers - 1
        if last:
            for copy in tables:
                copy.wait()
        for ref, at in ((x_ref, mine), (other_ref, theirs)):
            part = jnp.dot(
                ref[spots[layer], :, : held.shape[1]], held[layer], preferred_element_type=jnp.float32
            )
            if layer > 0:
                part = part + total[at, :]
            if not last:
                total[at, :] = part
                continue
            cosine, sine = cos_ref[at, :], sin_ref[at, :]
            for h, turn in enumerate(turned):
                a = part[:, h * HEAD : h * HEAD + half]
                b = part[:, h * HEAD + half : (h + 1) * HEAD]
                if turn:
                    a, b = a * cosine - b * sine, b * cosine + a * sine
                out_ref[at, h * HEAD : h * HEAD + half] = a.astype(jnp.bfloat16)
                out_ref[at, h * HEAD + half : (h + 1) * HEAD] = b.astype(jnp.bfloat16)


def project(x, other, arrays, slots, layers, spots, turned, tables, ids):
    tokens, depth, width = 2 * x.shape[1], 4 * arrays[0].shape[1], arrays[0].shape[2]
    vmem, left = pl.BlockSpec(memory_space=pltpu.VMEM), pl.BlockSpec(memory_space=pl.ANY)
    return pl.pallas_call(
        functools.partial(project_kernel, slots, turned),
        out_shape=jax.ShapeDtypeStruct((tokens + TAIL, width), jnp.bfloat16),
        in_specs=[pl.BlockSpec(memory_space=pltpu.SMEM)]
        + [vmem, vmem, left, left, vmem, vmem]
        + [left] * len(arrays),
        out_specs=vmem,
        scratch_shapes=[
            pltpu.VMEM((layers, depth, width), jnp.bfloat16),
            pltpu.VMEM((tokens, width), jnp.float32),
            pltpu.VMEM((tokens, HEAD // 2), jnp.float32),
            pltpu.VMEM((tokens, HEAD // 2), jnp.float32),
            pltpu.SemaphoreType.DMA((sum(len(blocks) for blocks in slots),)),
            pltpu.SemaphoreType.DMA((2,)),
        ],
        compiler_params=pltpu.CompilerParams(vmem_limit_bytes=12 * 1024 * 1024),
        cost_estimate=pl.CostEstimate(
            flops=2 * tokens * depth * layers * width,
            bytes_accessed=2 * layers * depth * width,
            transcendentals=0,
        ),
        name="project",
    )(spots, x, other, *in_hbm(tables), *ids, *in_hbm(arrays))


def attend_kernel(slots, layers, place, x_ref, other_ref, ids_ref, *refs):
    other_ids_ref, cos_hbm, sin_hbm, kv_hbm, old_hbm = refs[:5]
    pieces, refs = refs[5 : 5 + len(slots)], refs[5 + len(slots) :]
    own_ref, send_ref, held, total, q_ref, cos_ref, sin_ref, kv_ref, old_ref, sems, turns, ends = refs
    copies = fetch_layers(slots, 2 + layers, place, pieces, held, sems)
    tables = fetch_pair(cos_hbm, sin_hbm, cos_ref, sin_ref, turns)
    fetch = fetch_pair(kv_hbm, old_hbm, kv_ref, old_ref, ends)
    core, chip = place[0], place[1]
    step = own_ref.shape[1]
    tokens = q_ref.shape[0]
    behind = tokens
    first = core == 0
    ids = jnp.concatenate(
        [
            jnp.where(first, ids_ref[...], other_ids_ref[...]),
            jnp.where(first, other_ids_ref[...], ids_ref[...]),
        ],
        axis=1,
    ).astype(jnp.float32)
    query_ids = jnp.broadcast_to(ids, (128, tokens)).T[:, :1]
    half = HEAD // 2
    for layer in range(layers):
        for slot, copy in copies:
            if slot == layer:
                copy.wait()
        for ref, block in ((x_ref, 0), (other_ref, 1)):
            part = jnp.dot(
                ref[place[2 + layer], :, : held.shape[1]],
                held[layer],
                preferred_element_type=jnp.float32,
            )
            total[block] = part if layer == 0 else total[block] + part
    for copy in tables:
        copy.wait()
    for block, at in ((0, core), (1, 1 - core)):
        part = total[block]
        at = pl.ds(pl.multiple_of(at * step, step), step)
        cosine, sine = cos_ref[at, :], sin_ref[at, :]
        for h in range(GROUPS):
            a = part[:, h * HEAD : h * HEAD + half]
            b = part[:, h * HEAD + half : (h + 1) * HEAD]
            q_ref[at, h * HEAD : h * HEAD + half] = (a * cosine - b * sine).astype(jnp.bfloat16)
            q_ref[at, h * HEAD + half : (h + 1) * HEAD] = (b * cosine + a * sine).astype(
                jnp.bfloat16
            )
    for copy in fetch:
        copy.wait()
    old_ids = old_ref[behind : behind + TAIL, :].astype(jnp.float32)[:1]
    key_ids = jnp.concatenate([jnp.where(chip > 0, old_ids, -1.0), ids], axis=1)
    for m in range(tokens // step):
        low = m * step
        top = behind + (m + 1) * step
        span = top - low
        qpos = behind + m * step + lax.broadcasted_iota(jnp.int32, (step, span), 0)
        kpos = low + lax.broadcasted_iota(jnp.int32, (step, span), 1)
        same = query_ids[m * step : (m + 1) * step, :] == key_ids[:, low:top]
        allowed = same & (kpos <= qpos) & (qpos - kpos < WINDOW)
        keys = jnp.concatenate([old_ref[low:behind, :HEAD], kv_ref[: (m + 1) * step, :HEAD]], axis=0)
        values = jnp.concatenate(
            [old_ref[low:behind, HEAD:], kv_ref[: (m + 1) * step, HEAD:]], axis=0
        )
        for h in range(GROUPS):
            q = q_ref[m * step : (m + 1) * step, h * HEAD : (h + 1) * HEAD]
            scores = lax.dot_general(
                q, keys, (((1,), (1,)), ((), ())), preferred_element_type=jnp.float32
            )
            capped = CAP * jnp.tanh(scores * (1.0 / (CAP * math.sqrt(HEAD))))
            weights = jnp.where(allowed, jnp.exp(capped), 0.0)
            totals = jnp.sum(weights, axis=1, keepdims=True)
            mixed = jnp.dot(
                weights.astype(jnp.bfloat16), values, preferred_element_type=jnp.float32
            )
            result = (mixed / totals).astype(jnp.bfloat16)

            @pl.when(core == m)
            def _():
                own_ref[h] = result

            @pl.when(core != m)
            def _():
                send_ref[h] = result


def attend(x, other, arrays, slots, layers, place, tables, kv, old, ids):
    tokens, depth, width = 2 * x.shape[1], 4 * arrays[0].shape[1], arrays[0].shape[2]
    work = GROUPS * tokens * 2 * tokens * HEAD
    vmem, left = pl.BlockSpec(memory_space=pltpu.VMEM), pl.BlockSpec(memory_space=pl.ANY)
    return pl.pallas_call(
        functools.partial(attend_kernel, slots, layers),
        out_shape=[jax.ShapeDtypeStruct((GROUPS, tokens // 2, HEAD), jnp.bfloat16)] * 2,
        in_specs=[pl.BlockSpec(memory_space=pltpu.SMEM)] + [vmem] * 4 + [left] * (4 + len(arrays)),
        out_specs=[vmem] * 2,
        scratch_shapes=[
            pltpu.VMEM((layers, depth, width), jnp.bfloat16),
            pltpu.VMEM((2, tokens // 2, width), jnp.float32),
            pltpu.VMEM((tokens, width), jnp.bfloat16),
            pltpu.VMEM((tokens, HEAD // 2), jnp.float32),
            pltpu.VMEM((tokens, HEAD // 2), jnp.float32),
            pltpu.VMEM(kv.shape, jnp.bfloat16),
            pltpu.VMEM(old.shape, jnp.bfloat16),
            pltpu.SemaphoreType.DMA((sum(len(blocks) for blocks in slots),)),
            pltpu.SemaphoreType.DMA((2,)),
            pltpu.SemaphoreType.DMA((2,)),
        ],
        compiler_params=pltpu.CompilerParams(vmem_limit_bytes=20 * 1024 * 1024),
        cost_estimate=pl.CostEstimate(
            flops=4 * work, bytes_accessed=work // 256, transcendentals=0
        ),
        name="attend",
    )(place, x, other, *ids, *in_hbm(tables), *in_hbm([kv, old]), *in_hbm(arrays))


def head_of(own_ref, other_ref, core, head):
    return jnp.where(head // GROUPS == core, own_ref[head % GROUPS], other_ref[head % GROUPS])


def finish_kernel(slots, heads, marks, own_hbm, other_hbm, gain_ref, hid_hbm, *refs):
    pieces = refs[: len(slots)]
    out_hbm, held, own_ref, other_ref, hid_ref, sum_ref, out_ref, sems, ends = refs[len(slots) :]
    fetch = fetch_pair(own_hbm, other_hbm, own_ref, other_ref, ends)
    copies = fetch_layers(slots, heads + 1, marks, pieces, held, sems)
    hidden = pltpu.make_async_copy(hid_hbm, hid_ref, ends.at[2])
    hidden.start()
    for copy in fetch:
        copy.wait()
    tokens, width = sum_ref.shape
    tile = next(t for t in (768, 512, 256, 128, width) if width % t == 0)
    square = jnp.zeros((tokens, 1), jnp.float32)
    for s in range(heads):
        for slot, copy in copies:
            if slot == s:
                copy.wait()
        att = head_of(own_ref, other_ref, marks[heads], marks[s])
        for n in range(width // tile):
            part = slice(n * tile, (n + 1) * tile)
            total = jnp.dot(att, held[s, :, part], preferred_element_type=jnp.float32)
            if s > 0:
                total = sum_ref[:, part] + total
            sum_ref[:, part] = total
            if s == heads - 1:
                square = square + jnp.sum(total * total, axis=1, keepdims=True)
    scale = lax.rsqrt(square / width + EPS)
    hidden.wait()
    step = 64
    stores = []
    for m in range(tokens // step):
        rows = slice(m * step, (m + 1) * step)
        branch = sum_ref[rows, :] * scale[rows] * gain_ref[...]
        out_ref[rows, :] = (hid_ref[rows, :].astype(jnp.float32) + branch).astype(jnp.bfloat16)
        stores.append(
            pltpu.make_async_copy(out_ref.at[rows, :], out_hbm.at[rows, :], ends.at[3 + m])
        )
        stores[-1].start()
    for store in stores:
        store.wait()


def finish(own, other, arrays, slots, marks, heads, rows, gain, hidden):
    tokens, width = hidden.shape
    vmem, left = pl.BlockSpec(memory_space=pltpu.VMEM), pl.BlockSpec(memory_space=pl.ANY)
    return pl.pallas_call(
        functools.partial(finish_kernel, slots, heads),
        out_shape=jax.ShapeDtypeStruct((tokens, width), jnp.bfloat16),
        in_specs=[pl.BlockSpec(memory_space=pltpu.SMEM), left, left, vmem, left]
        + [left] * len(arrays),
        out_specs=left,
        scratch_shapes=[
            pltpu.VMEM((heads, rows, width), jnp.bfloat16),
            pltpu.VMEM(own.shape, jnp.bfloat16),
            pltpu.VMEM(own.shape, jnp.bfloat16),
            pltpu.VMEM((tokens, width), jnp.bfloat16),
            pltpu.VMEM((tokens, width), jnp.float32),
            pltpu.VMEM((tokens, width), jnp.bfloat16),
            pltpu.SemaphoreType.DMA((sum(len(blocks) for blocks in slots),)),
            pltpu.SemaphoreType.DMA((3 + tokens // 64,)),
        ],
        compiler_params=pltpu.CompilerParams(vmem_limit_bytes=18 * 1024 * 1024),
        cost_estimate=pl.CostEstimate(
            flops=2 * tokens * rows * heads * width,
            bytes_accessed=2 * rows * heads * width,
            transcendentals=0,
        ),
        name="finish",
    )(marks, own, other, gain, *in_hbm([hidden]), *arrays)


def per_device(hidden_in, segment_ids, pre_gain, w_qkv, w_out, post_gain):
    return layer(hidden_in, segment_ids, pre_gain, w_qkv, w_out, post_gain)


def layer(hidden_in, segment_ids, pre_gain, w_qkv, w_out, post_gain):
    tok_rows, model = hidden_in.shape[1:]
    seq_count = lax.axis_size("seq")
    line_count = seq_count // 4
    seq_index = lax.axis_index("seq")
    plane = lax.axis_index("batch")
    core, pair, line = seq_index % 2, (seq_index // 2) % 2, seq_index // 4
    chip = seq_index // 2
    chip_rows = 2 * tok_rows

    half_rows = w_out.shape[0] // 2
    came = swap_core(w_qkv)
    own_kv, own_q, kv_unit, q_unit, out_unit = prepare(w_qkv, came, w_out, core, plane)
    first_pos, out_unit, pre_gain = lax.optimization_barrier(
        (chip * chip_rows, out_unit, pre_gain)
    )
    kv_pieces = gather_near(own_kv, kv_unit, plane, pair, line_count, "1")
    q_pieces = gather_wide(own_q, q_unit, plane, pair, line_count)
    out_own = w_out.reshape(2, half_rows, model)
    out_pieces = gather_near(out_own, out_unit, plane, pair, line_count, "3")

    cosine, sine = rotary_tables(first_pos + jnp.arange(chip_rows, dtype=jnp.int32))
    normed = norm(hidden_in[0], pre_gain, [cosine, sine], line_count)
    normed_other = swap_core(normed)
    ids = (segment_ids, swap_core(segment_ids))

    backs = list(range(line_count))
    layers = [(line - back + line_count) % line_count for back in backs]

    def laid(pieces):
        arrays = [block for block, _ in pieces]
        slots = tuple(tuple(back for back, _, _ in blocks) for _, blocks in pieces)
        rows = arrays[0].shape[1]
        return arrays, slots, [(y * 2 + h) * rows for _, blocks in pieces for _, y, h in blocks]

    def scalars(entries):
        return jnp.stack([jnp.asarray(entry, jnp.int32) for entry in entries])

    arrays, slots, spots = laid(kv_pieces)
    kv = project(
        normed,
        normed_other,
        arrays,
        slots,
        line_count,
        scalars(layers + spots + [core]),
        turned=(True, False),
        tables=(cosine, sine),
        ids=ids,
    )
    old = from_chip_behind(kv, 1)
    arrays, slots, spots = laid(q_pieces)
    att_own, att_send = attend(
        normed,
        normed_other,
        arrays,
        slots,
        line_count,
        scalars([core, chip] + layers + spots),
        (cosine, sine),
        kv,
        old,
        ids,
    )
    att_other = swap_core(att_send)

    swapped = [swap_core(block) for block, _ in out_pieces]

    offsets, arrays, slots = [], [], []
    for (block, blocks), other in zip(out_pieces, swapped):
        for array, c in zip(in_hbm([block, other]), (core, 1 - core)):
            arrays.append(array)
            slots.append(tuple(back for back, _, _ in blocks))
            offsets += [((y * 2 + c) * 2 + h) * half_rows for _, y, h in blocks]
    done = finish(
        att_own,
        att_other,
        arrays,
        tuple(slots),
        scalars(layers + [core] + offsets),
        line_count,
        8 * half_rows,
        post_gain[None, :],
        hidden_in[0],
    )
    return done[None]


BY_BATCH = ()


def from_behind(block, axis, distance):
    devices = range(lax.axis_size(axis))
    route = [(i - distance, i) for i in devices if i - distance in devices]
    return lax.ppermute(block, axis, route)


def rotary(values, positions, leading):
    head_size = values.shape[-1]
    half_dim = head_size // 2
    inverse = 1.0 / 10000.0 ** (jnp.arange(half_dim, dtype=jnp.float32) * 2.0 / head_size)
    angles = positions.astype(jnp.float32)[:, None] * inverse[None, :]
    shape = (
        (1,) * leading + (positions.shape[0],) + (1,) * (values.ndim - 2 - leading) + (half_dim,)
    )
    cosine = jnp.cos(angles).reshape(shape)
    sine = jnp.sin(angles).reshape(shape)
    first_half = values[..., :half_dim]
    second_half = values[..., half_dim:]
    return jnp.concatenate(
        [first_half * cosine - second_half * sine, second_half * cosine + first_half * sine],
        axis=-1,
    )


def attend_block(states, queries, key_block, value_block, query_pos, key_pos, starts):
    running, totals = states
    scores = jnp.einsum(
        "qhgd,khd->qhgk", queries, key_block, preferred_element_type=jnp.float32
    ) * (1.0 / math.sqrt(HEAD))
    capped = CAP * jnp.tanh(scores / CAP)
    allowed = (
        (key_pos[None, :] <= query_pos[:, None])
        & (query_pos[:, None] - key_pos[None, :] < WINDOW)
        & (key_pos[None, :] >= starts[:, None])
    )
    weights = jnp.where(allowed[:, None, None, :], jnp.exp(capped), 0.0)
    totals = totals + jnp.sum(weights, axis=-1)
    running = running + jnp.einsum(
        "qhgk,khd->qhgd",
        weights.astype(jnp.bfloat16),
        value_block,
        preferred_element_type=jnp.float32,
    )
    return (running, totals)


def per_device_general(hidden_in, segment_ids, pre_gain, w_qkv, w_out, post_gain):
    tok_rows = hidden_in.shape[1]
    seq_count = lax.axis_size("seq")
    seq_index = lax.axis_index("seq")
    groups = Q_HEADS // KV_HEADS
    positions = seq_index * tok_rows + jnp.arange(tok_rows, dtype=jnp.int32)
    widened = hidden_in[0].astype(jnp.float32)
    normed = rms_scale(widened, pre_gain).astype(jnp.bfloat16)
    columns = normed
    projected = jnp.dot(
        columns,
        lax.all_gather(w_qkv, "seq", axis=0, tiled=True),
        preferred_element_type=jnp.float32,
    )
    queries = rotary(
        projected[:, : Q_HEADS * HEAD].reshape(tok_rows, KV_HEADS, groups, HEAD), positions, 0
    ).astype(jnp.bfloat16)
    key_rows = rotary(
        projected[:, Q_HEADS * HEAD : (Q_HEADS + KV_HEADS) * HEAD].reshape(
            tok_rows, KV_HEADS, HEAD
        ),
        positions,
        0,
    ).astype(jnp.bfloat16)
    value_rows = (
        projected[:, (Q_HEADS + KV_HEADS) * HEAD :]
        .reshape(tok_rows, KV_HEADS, HEAD)
        .astype(jnp.bfloat16)
    )
    doc_numbers = jnp.arange(DOCS, dtype=jnp.int32)
    matches = segment_ids[0][:, None] == doc_numbers[None, :]
    local_first = jnp.min(jnp.where(matches, positions[:, None], seq_count * tok_rows), axis=0)
    first_pos = lax.pmin(local_first, "seq")
    starts = jnp.sum(jnp.where(matches, first_pos[None, :], 0), axis=1)
    states = (
        jnp.zeros((tok_rows, KV_HEADS, groups, HEAD), jnp.float32),
        jnp.zeros((tok_rows, KV_HEADS, groups), jnp.float32),
    )
    states = attend_block(states, queries, key_rows, value_rows, positions, positions, starts)
    longest = min(2 * seq_count * tok_rows // DOCS, WINDOW)
    hop_count = min(-(-(longest - 1) // tok_rows), seq_count - 1)

    def relay_step(hop_index, carried):
        moving_keys, moving_values, running, totals = carried
        moving_keys, moving_values = from_behind((moving_keys, moving_values), "seq", 1)
        running, totals = attend_block(
            (running, totals),
            queries,
            moving_keys,
            moving_values,
            positions,
            positions - hop_index * tok_rows,
            starts,
        )
        return (moving_keys, moving_values, running, totals)

    carried = lax.fori_loop(
        1, hop_count + 1, relay_step, (key_rows, value_rows, states[0], states[1])
    )
    states = (carried[2], carried[3])
    running, totals = states
    attended = (running / totals[..., None]).astype(jnp.bfloat16).reshape(tok_rows, Q_HEADS * HEAD)
    columns = attended
    branch = jnp.dot(
        columns,
        lax.all_gather(w_out, "seq", axis=0, tiled=True),
        preferred_element_type=jnp.float32,
    )
    return (widened + rms_scale(branch, post_gain)).astype(jnp.bfloat16)[None]


def solution(mesh):
    seq_count, planes = mesh.shape["seq"], mesh.shape["batch"]
    special = seq_count == 4 * Q_HEADS == DOCS and planes == 2 == KV_HEADS and Q_HEADS == 4
    placed = (P("batch", "seq", None), P("batch", "seq"), P(), P("seq", None), P("seq", None), P())
    return jax.shard_map(
        per_device if special else per_device_general,
        mesh=mesh,
        in_specs=placed,
        out_specs=P("batch", "seq", None),
        check_vma=False,
    )
```
